64 devices in a mesh: dp: 4 (over x, y), ep: 16 (over z, core).
Axes of the slice: x: 2, y: 2, z: 8, core: 2. Of those that a mesh axis runs over, the one named last changes fastest.
The devices are a block of a 4x4x8 slice.
Arguments:
- act_in: bfloat16 [8192, 2048], P(('dp', 'ep')), parts along dimension 0
- router_w: bfloat16 [2048, 64], replicated
- expert_ids: int32 [8192, 8], P(('dp', 'ep')), parts along dimension 0
- w_gate: bfloat16 [64, 2048, 1024], P('ep')
- w_up: bfloat16 [64, 2048, 1024], P('ep')
- w_down: bfloat16 [64, 1024, 2048], P('ep')
Outputs:
- output: bfloat16 [8192, 2048], P(('dp', 'ep')), parts along dimension 0
There are 4 independent parts. The reference program is written for one: setup_inputs(seed, part) draws one part's arguments, and reference() takes and returns one part's arrays. A program takes and returns all parts, laid end to end along the dimension named above; an argument that names none is the same for every part.
All inputs are finite; a program needn't handle non-finite values.
Results may differ from the reference program's by a relative error of at most 0.00133.
Values are sent between devices in bfloat16 or wider.
A program may use at most 768 MiB of HBM per device.

```python
import jax
import jax.numpy as jnp
from jax import lax

GROUP_SIZE = 16
TOKENS = 128
MODEL_DIM = 2048
FFN_DIM = 1024
EXPERTS = 64
TOP_K = 8

MICRO_LEN = TOKENS // 2
MEAN_LOAD = MICRO_LEN * TOP_K // EXPERTS
CAPACITY = MEAN_LOAD + MEAN_LOAD // 2
BUF_LEN = GROUP_SIZE * CAPACITY


def run_index(run_ends):
    return jnp.searchsorted(run_ends, jnp.arange(MICRO_LEN * TOP_K, dtype=jnp.int32), side='right').astype(jnp.int32)


def draw_routing(route_key):
    pair_key, load_key, order_key = jax.random.split(route_key, 3)
    expert_order = jax.random.permutation(pair_key, EXPERTS)
    shifts = jax.random.randint(load_key, (GROUP_SIZE, 2, EXPERTS // 2), 0, MEAN_LOAD // 2 + 1)
    shifts = jnp.where(jnp.arange(EXPERTS // 2) == 0, MEAN_LOAD // 2, shifts)
    counts = jnp.stack([MEAN_LOAD + shifts, MEAN_LOAD - shifts], axis=-1).reshape(GROUP_SIZE, 2, EXPERTS)
    run_ids = jax.vmap(jax.vmap(run_index))(jnp.cumsum(counts, axis=-1))
    chosen = jnp.swapaxes(expert_order[run_ids].reshape(GROUP_SIZE, 2, TOP_K, MICRO_LEN), 2, 3)
    scores = jax.random.randint(order_key, (GROUP_SIZE, 2, MICRO_LEN), 0, MICRO_LEN) * MICRO_LEN + jnp.arange(MICRO_LEN)
    token_order = jnp.broadcast_to(jnp.argsort(scores, axis=-1)[..., None], chosen.shape)
    chosen = jnp.take_along_axis(chosen, token_order, axis=2)
    return chosen.reshape(GROUP_SIZE * TOKENS, TOP_K).astype(jnp.int32)


def setup_inputs(seed: int = 0, part: int = 0) -> dict:
    part_key = jax.random.fold_in(jax.random.key(seed), part)
    act_key, route_key = jax.random.split(part_key, 2)
    gate_key, up_key, down_key, router_key = jax.random.split(jax.random.key(seed + 1), 4)
    act_in = jax.random.normal(act_key, (GROUP_SIZE * TOKENS, MODEL_DIM), jnp.float32)
    router_w = jax.random.normal(router_key, (MODEL_DIM, EXPERTS), jnp.float32) * (1.5 / MODEL_DIM ** 0.5)
    w_gate = jax.random.normal(gate_key, (EXPERTS, MODEL_DIM, FFN_DIM), jnp.float32) / MODEL_DIM ** 0.5
    w_up = jax.random.normal(up_key, (EXPERTS, MODEL_DIM, FFN_DIM), jnp.float32) / MODEL_DIM ** 0.5
    w_down = jax.random.normal(down_key, (EXPERTS, FFN_DIM, MODEL_DIM), jnp.float32) / FFN_DIM ** 0.5
    return {
        'act_in': act_in.astype(jnp.bfloat16),
        'router_w': router_w.astype(jnp.bfloat16),
        'expert_ids': draw_routing(route_key),
        'w_gate': w_gate.astype(jnp.bfloat16),
        'w_up': w_up.astype(jnp.bfloat16),
        'w_down': w_down.astype(jnp.bfloat16),
    }


def expert_block(tok_rows, gate_mat, up_mat, down_mat):
    gate_h = jnp.dot(tok_rows, gate_mat, preferred_element_type=jnp.float32)
    up_h = jnp.dot(tok_rows, up_mat, preferred_element_type=jnp.float32)
    hidden = (jax.nn.silu(gate_h) * up_h).astype(jnp.bfloat16)
    return jnp.dot(hidden, down_mat, preferred_element_type=jnp.float32).astype(jnp.bfloat16)


def micro_layer(tok_rows, pair_ids, gate_vals, w_gate, w_up, w_down):
    flat_ids = pair_ids.reshape(-1)
    num_pairs = flat_ids.shape[0]
    sort_order = jnp.argsort(flat_ids, stable=True)
    sorted_ids = flat_ids[sort_order]
    counts = jnp.bincount(flat_ids, length=EXPERTS)
    starts = jnp.cumsum(counts) - counts
    pair_rank = jnp.arange(num_pairs) - starts[sorted_ids]
    pair_slot = jnp.zeros_like(sort_order).at[sort_order].set(sorted_ids * BUF_LEN + pair_rank)
    padded_order = jnp.concatenate([sort_order, jnp.zeros_like(sort_order[:BUF_LEN])])

    def one_expert(expert):
        pick_rows = lax.dynamic_slice(padded_order, (starts[expert],), (BUF_LEN,))
        return expert_block(tok_rows[pick_rows // TOP_K], w_gate[expert], w_up[expert], w_down[expert])

    expert_out = lax.map(one_expert, jnp.arange(EXPERTS))
    pair_out = expert_out.reshape(EXPERTS * BUF_LEN, MODEL_DIM)[pair_slot]
    pair_out = pair_out.reshape(num_pairs // TOP_K, TOP_K, MODEL_DIM).astype(jnp.float32)
    return jnp.sum(gate_vals[..., None] * pair_out, axis=1).astype(jnp.bfloat16)


def reference(act_in, router_w, expert_ids, w_gate, w_up, w_down):
    logits = jnp.dot(act_in, router_w, preferred_element_type=jnp.float32)
    gate_vals = jax.nn.softmax(jnp.take_along_axis(logits, expert_ids, axis=1), axis=-1)
    tok_mb = jnp.swapaxes(act_in.reshape(GROUP_SIZE, 2, MICRO_LEN, MODEL_DIM), 0, 1).reshape(2, GROUP_SIZE * MICRO_LEN, MODEL_DIM)
    ids_mb = jnp.swapaxes(expert_ids.reshape(GROUP_SIZE, 2, MICRO_LEN, TOP_K), 0, 1).reshape(2, GROUP_SIZE * MICRO_LEN, TOP_K)
    gate_mb = jnp.swapaxes(gate_vals.reshape(GROUP_SIZE, 2, MICRO_LEN, TOP_K), 0, 1).reshape(2, GROUP_SIZE * MICRO_LEN, TOP_K)

    def run_micro(micro_args):
        return micro_layer(micro_args[0], micro_args[1], micro_args[2], w_gate, w_up, w_down)

    out_mb = lax.map(run_micro, (tok_mb, ids_mb, gate_mb))
    return jnp.swapaxes(out_mb.reshape(2, GROUP_SIZE, MICRO_LEN, MODEL_DIM), 0, 1).reshape(GROUP_SIZE * TOKENS, MODEL_DIM)
```

```python
import functools

import jax
import jax.numpy as jnp
from jax import lax
from jax.experimental import pallas as pl
from jax.experimental.pallas import tpu as pltpu
from jax.sharding import PartitionSpec as P

MESH = pl.DeviceIdType.MESH
F32 = jnp.float32
BF16 = jnp.bfloat16

POS = {4: 0, -4: 0, 0: 1, -3: 2, 3: 3, -2: 4, 2: 5, -1: 6, 1: 7}
SIGN = (1, -1)
BACK = ((4, 0), (3, 1), (3, 0), (2, 1), (2, 0), (1, 1), (1, 0))
GU_TILE = 256
DN_TILE = 1024


def dot(a, b):
    return jnp.dot(a, b, preferred_element_type=F32)


def layer_kernel(group, ids_hbm, rw_hbm, x_hbm, wg_hbm, wu_hbm, wd_hbm, out_hbm,
                 xg, meta, ids_v, rw_v, tp, xe, hid, eo, cm, part, sib, inb, outv, wgu, wdn,
                 ag_s, ag_r, dx_s, dx_r, mt_s, mt_r, dm_s, dm_r, rs_s, rs_r, sb_s, sb_r,
                 gu_sem, dn_sem, ld_sem, st_sem):
    micro = 64
    half = 32
    me = lax.axis_index('ep')
    core = lax.rem(me, 2)
    other = 1 - core
    nbr = (lax.rem(me + 2, group), lax.rem(me + group - 2, group))
    sibling = me + 1 - 2 * core
    local_experts = wg_hbm.shape[0]
    slots = xe.shape[1] // 4

    def remote(src, dst, ssem, rsem, dev):
        return pltpu.make_async_remote_copy(src_ref=src, dst_ref=dst, send_sem=ssem, recv_sem=rsem,
                                            device_id={'ep': dev}, device_id_type=MESH)

    def gu_copies(e, f):
        cols = pl.ds(f * GU_TILE, GU_TILE)
        return (pltpu.make_async_copy(wg_hbm.at[e, :, cols], wgu.at[f, 0], gu_sem.at[f, 0]),
                pltpu.make_async_copy(wu_hbm.at[e, :, cols], wgu.at[f, 1], gu_sem.at[f, 1]))

    def dn_copy(e, n):
        return pltpu.make_async_copy(wd_hbm.at[e, :, pl.ds(n * DN_TILE, DN_TILE)], wdn.at[n], dn_sem.at[n])

    def x_rows(m, pos, c, start, size):
        row = pl.multiple_of((pos % 2) * 2 * micro + c * micro + start, half)
        return xg.at[m, pos // 2, pl.ds(row, size)]

    def ag_copy(m, d, k, piece):
        src = x_rows(m, POS[-SIGN[d] * k], core, piece * half, half)
        dst = x_rows(m, POS[-SIGN[d] * (k + 1)], core, piece * half, half)
        return remote(src, dst, ag_s.at[m, d, k, piece], ag_r.at[m, d, k, piece], nbr[d])

    def ag_has(d, k, piece):
        return k < 3 or piece == d

    def dx_copy(m, pos, c):
        ref = x_rows(m, pos, c, 0, micro)
        return remote(ref, ref, dx_s.at[m, pos], dx_r.at[m, pos], sibling)

    def mt_copy(d, k):
        return remote(meta.at[POS[-SIGN[d] * k], core], meta.at[POS[-SIGN[d] * (k + 1)], core],
                      mt_s.at[d, k], mt_r.at[d, k], nbr[d])

    def mt_has(d, k):
        return k < 3 or d == 0

    def dm_copy(pos, c):
        return remote(meta.at[pos, c], meta.at[pos, c], dm_s.at[pos], dm_r.at[pos], sibling)

    def send_own(m):
        for piece in range(2):
            for d in range(2):
                ag_copy(m, d, 0, piece).start()
        dx_copy(m, POS[0], core).start()

    def ag_event(m, k, piece):
        for d in range(2):
            if ag_has(d, k, piece):
                ag_copy(m, d, k, piece).wait_recv()
                if k < 3 and ag_has(d, k + 1, piece):
                    ag_copy(m, d, k + 1, piece).start()
        if piece == 1:
            for pos in ((POS[4],) if k == 3 else (POS[-(k + 1)], POS[k + 1])):
                dx_copy(m, pos, core).start()

    def mt_event(k):
        for d in range(2):
            if mt_has(d, k):
                mt_copy(d, k).wait_recv()
                if k < 3 and mt_has(d, k + 1):
                    mt_copy(d, k + 1).start()
                dm_copy(POS[-SIGN[d] * (k + 1)], core).start()

    def make_meta():
        for m in range(2):
            rows = x_rows(m, POS[0], core, 0, micro)
            tp[0, m * micro:(m + 1) * micro, 0:rw_v.shape[1]] = dot(rows[...], rw_v[...])
        tp[1, :, 0:8] = ids_v[...].astype(F32)
        logits = tp[0].T
        ids = tp[1].T[0:8]
        expert = lax.broadcasted_iota(jnp.int32, (rw_v.shape[1], 2 * micro), 0).astype(F32)
        logits = logits[0:rw_v.shape[1]]
        picked = []
        for j in range(8):
            picked.append(jnp.sum(jnp.where(expert == ids[j:j + 1], logits, 0.0), axis=0, keepdims=True))
        picked = jnp.concatenate(picked, axis=0)
        top = jnp.exp(picked - jnp.max(picked, axis=0, keepdims=True))
        gates = top / jnp.sum(top, axis=0, keepdims=True)
        both = jnp.concatenate([ids, gates], axis=0)
        turned = pltpu.roll(both, micro, 1)
        mine = lax.broadcasted_iota(jnp.int32, both.shape, 1) // micro == core
        for m in range(2):
            meta[POS[0], core, m] = jnp.where(mine, jnp.where(core == m, both, turned), 0.0)

    def gather(m, p):
        token = 4 * micro
        info = jnp.concatenate([meta[2 * p, 0, m] + meta[2 * p, 1, m],
                                meta[2 * p + 1, 0, m] + meta[2 * p + 1, 1, m]], axis=1)
        ids, gates = info[0:8], info[8:16]
        chosen, weight = [], []
        for e in range(local_experts):
            hit = ids == (me * local_experts + e).astype(F32)
            chosen.append(jnp.sum(jnp.where(hit, 1.0, 0.0), axis=0, keepdims=True))
            weight.append(jnp.sum(jnp.where(hit, gates, 0.0), axis=0, keepdims=True))
        stacked = jnp.concatenate(chosen + [jnp.zeros((16 - local_experts, token), F32)], axis=0)
        row = lax.broadcasted_iota(jnp.int32, (token, token), 0)
        col = lax.broadcasted_iota(jnp.int32, (token, token), 1)
        before = jnp.where(row < col, 1.0, 0.0).astype(BF16)
        eye = jnp.where(row == col, 1.0, 0.0).astype(BF16)
        rank = dot(stacked.astype(BF16), before)
        slot = lax.broadcasted_iota(jnp.int32, (slots, token), 0).astype(F32)
        pick, mix = [], []
        for e in range(local_experts):
            place = jnp.where(chosen[e] > 0.5, rank[e:e + 1], -1.0)
            at = slot == place
            pick.append(jnp.where(at, 1.0, 0.0))
            mix.append(jnp.where(at, weight[e], 0.0))
        pick = jnp.concatenate(pick, axis=0).astype(BF16)
        rest = jnp.concatenate(mix, axis=0)
        for i in range(3):
            term = rest.astype(BF16)
            rest = rest - term.astype(F32)
            turned = lax.dot_general(eye, term, (((1,), (1,)), ((), ())), preferred_element_type=F32)
            cm[p, i] = turned.astype(BF16)
        for n in range(0, xg.shape[-1], 512):
            rows = dot(pick, xg[m, p, :, n:n + 512]).astype(BF16)
            for e in range(local_experts):
                xe[e, pl.ds(pl.multiple_of(p * slots, 16), slots), n:n + 512] = rows[e * slots:(e + 1) * slots]

    def expert(e, more):
        nxt = lax.rem(e + 1, local_experts)
        for f in range(4):
            for cp in gu_copies(e, f):
                cp.wait()
            a = dot(xe[e], wgu[f, 0])
            b = dot(xe[e], wgu[f, 1])
            hid[:, f * GU_TILE:(f + 1) * GU_TILE] = (a * jax.nn.sigmoid(a) * b).astype(BF16)

            @pl.when(more)
            def _():
                for cp in gu_copies(nxt, f):
                    cp.start()
        for n in range(2):
            dn_copy(e, n).wait()
            for s in range(0, DN_TILE, 512):
                o = dot(hid[...], wdn[n, :, s:s + 512]).astype(BF16)
                for p in range(4):
                    eo[p, pl.ds(pl.multiple_of(e * slots, 16), slots),
                       n * DN_TILE + s:n * DN_TILE + s + 512] = o[p * slots:(p + 1) * slots]

            @pl.when(more)
            def _():
                dn_copy(nxt, n).start()

    def combine(pos):
        p, top = pos // 2, (pos % 2) * 2 * micro

        @pl.loop(0, xg.shape[-1] // 512)
        def _(i):
            cols = pl.ds(pl.multiple_of(i * 512, 512), 512)
            o = eo[p, :, cols]
            acc = dot(cm[p, 0, top:top + 2 * micro], o)
            acc = acc + dot(cm[p, 1, top:top + 2 * micro], o)
            acc = acc + dot(cm[p, 2, top:top + 2 * micro], o)
            part[pos, 0, :, cols] = acc[:micro]
            part[pos, 1, :, cols] = acc[micro:]

    def sb_copy(m, pos):
        return remote(part.at[pos, other], sib.at[m, pos], sb_s.at[m, pos], sb_r.at[m, pos], sibling)

    def back_item(d, j):
        dist, rows = BACK[j]
        return POS[SIGN[d] * dist], (rows if d == 0 else 1 - rows)

    def rs_copy(m, d, j):
        pos, r = back_item(d, j)
        return remote(part.at[pos, core, pl.ds(r * half, half)], inb.at[m, d, j],
                      rs_s.at[m, d, j], rs_r.at[m, d, j], nbr[d])

    here = set()

    def need_sib(m, pos):
        if (m, pos) not in here:
            here.add((m, pos))
            sb_copy(m, pos).wait_recv()

    def back(m, j):
        for d in range(2):
            pos, r = back_item(d, j)
            need_sib(m, pos)
            rows = pl.ds(r * half, half)
            acc = part[pos, core, rows] + sib[m, pos, rows]
            if j >= 2:
                rs_copy(m, d, j - 2).wait_recv()
                acc = acc + inb[m, d, j - 2]
            part[pos, core, rows] = acc
            rs_copy(m, d, j).start()

    def st_copy(m, r):
        rows = pl.ds(m * micro + r * half, half)
        return pltpu.make_async_copy(outv.at[rows], out_hbm.at[rows], st_sem.at[m, r])

    def finish(m, r):
        pos = POS[0]
        need_sib(m, pos)
        rows = pl.ds(r * half, half)
        acc = part[pos, core, rows] + sib[m, pos, rows]
        for d in range(2):
            j = 5 if (r == 1) == (d == 0) else 6
            if (m, d, j) not in here:
                here.add((m, d, j))
                rs_copy(m, d, j).wait_recv()
            acc = acc + inb[m, d, j]
        outv[pl.ds(m * micro + r * half, half)] = acc.astype(BF16)
        st_copy(m, r).start()

    def combine_send(m, pos):
        combine(pos)
        sb_copy(m, pos).start()

    def part_free(m, pos):
        sb_copy(m, pos).wait_send()
        for d in range(2):
            for j in range(7):
                if back_item(d, j)[0] == pos:
                    rs_copy(m, d, j).wait_send()

    def pair_wait(m, p):
        for pos in (2 * p, 2 * p + 1):
            dx_copy(m, pos, other).wait_recv()
            if m == 0:
                dm_copy(pos, other).wait_recv()

    loads = [pltpu.make_async_copy(x_hbm.at[pl.ds(m * micro, micro)], x_rows(m, POS[0], core, 0, micro), ld_sem.at[m])
             for m in range(2)]
    loads.append(pltpu.make_async_copy(ids_hbm, ids_v, ld_sem.at[2]))
    loads.append(pltpu.make_async_copy(rw_hbm, rw_v, ld_sem.at[3]))
    for cp in loads:
        cp.start()

    barrier = pltpu.get_barrier_semaphore()
    for dev in (nbr[0], nbr[1], sibling):
        pl.semaphore_signal(barrier, inc=1, device_id={'ep': dev}, device_id_type=MESH)
    for f in range(4):
        for cp in gu_copies(0, f):
            cp.start()
    for n in range(2):
        dn_copy(0, n).start()
    loads[0].wait()
    pl.semaphore_wait(barrier, 3)

    send_own(0)
    for cp in loads[1:]:
        cp.wait()
    make_meta()
    for d in range(2):
        mt_copy(d, 0).start()
    dm_copy(POS[0], core).start()

    ag_event(0, 0, 0)
    ag_event(0, 0, 1)
    mt_event(0)
    ag_event(0, 1, 0)
    ag_event(0, 1, 1)
    mt_event(1)
    pair_wait(0, 3)
    gather(0, 3)
    ag_event(0, 2, 0)
    ag_event(0, 2, 1)
    mt_event(2)
    send_own(1)
    pair_wait(0, 2)
    gather(0, 2)
    pair_wait(0, 1)
    gather(0, 1)
    ag_event(0, 3, 0)
    ag_event(0, 3, 1)
    mt_event(3)
    pair_wait(0, 0)
    gather(0, 0)

    @pl.loop(0, local_experts)
    def _(e):
        expert(e, e >= 0)
        for i, (k, piece) in enumerate(((0, 0), (0, 1), (1, 0), (1, 1))):
            @pl.when(e == i)
            def _():
                ag_event(1, k, piece)

    combine_send(0, POS[4])
    combine_send(0, POS[-3])
    combine_send(0, POS[3])
    ag_event(1, 2, 0)
    ag_event(1, 2, 1)
    back(0, 0)
    back(0, 1)
    for pos in (4, 5, 6, 7, 1):
        combine_send(0, pos)
    ag_event(1, 3, 0)
    ag_event(1, 3, 1)
    for p in range(4):
        pair_wait(1, p)

    @pl.loop(0, 4)
    def _(p):
        gather(1, p)

    for j in range(2, 7):
        for d in range(2):
            need_sib(0, back_item(d, j)[0])

    @pl.loop(0, local_experts)
    def _(e):
        expert(e, e < local_experts - 1)
        for i, j in ((0, 2), (2, 3), (3, 4)):
            @pl.when(e == i)
            def _():
                back(0, j)

    back(0, 5)
    for pos in (0, 2, 3):
        part_free(0, pos)
        combine_send(1, pos)
    back(0, 6)
    back(1, 0)
    back(1, 1)
    for pos in (4, 5):
        part_free(0, pos)
        combine_send(1, pos)
    finish(0, 0)
    finish(0, 1)
    for pos in (6, 7, 1):
        part_free(0, pos)
        combine_send(1, pos)
    for j in range(2, 7):
        back(1, j)
    finish(1, 0)
    finish(1, 1)

    for m in range(2):
        for d in range(2):
            for k in range(4):
                for piece in range(2):
                    if ag_has(d, k, piece):
                        ag_copy(m, d, k, piece).wait_send()
        for pos in range(8):
            dx_copy(m, pos, core).wait_send()
    for d in range(2):
        for k in range(4):
            if mt_has(d, k):
                mt_copy(d, k).wait_send()
    for pos in range(8):
        dm_copy(pos, core).wait_send()
        part_free(1, pos)
    for m in range(2):
        for r in range(2):
            st_copy(m, r).wait()


def solution(mesh):
    group = mesh.shape['ep']

    def device_fn(act_in, router_w, expert_ids, w_gate, w_up, w_down):
        tokens, dim = act_in.shape
        local_experts, _, ffn = w_gate.shape
        micro = tokens // 2
        half = micro // 2
        mean_load = micro * expert_ids.shape[1] // (local_experts * group)
        cap = mean_load + mean_load // 2
        slots = 4 * cap
        dma = pltpu.SemaphoreType.DMA
        scratch = [
            pltpu.VMEM((2, 4, 4 * micro, dim), BF16),
            pltpu.VMEM((8, 2, 2, 16, 2 * micro), F32),
            pltpu.VMEM(expert_ids.shape, jnp.int32),
            pltpu.VMEM(router_w.shape, BF16),
            pltpu.VMEM((2, tokens, 128), F32),
            pltpu.VMEM((local_experts, 4 * slots, dim), BF16),
            pltpu.VMEM((4 * slots, ffn), BF16),
            pltpu.VMEM((4, local_experts * slots, dim), BF16),
            pltpu.VMEM((4, 3, 4 * micro, local_experts * slots), BF16),
            pltpu.VMEM((8, 2, micro, dim), F32),
            pltpu.VMEM((2, 8, micro, dim), F32),
            pltpu.VMEM((2, 2, 7, half, dim), F32),
            pltpu.VMEM((tokens, dim), BF16),
            pltpu.VMEM((4, 2, dim, GU_TILE), BF16),
            pltpu.VMEM((2, ffn, DN_TILE), BF16),
            dma((2, 2, 4, 2)), dma((2, 2, 4, 2)),
            dma((2, 8)), dma((2, 8)),
            dma((2, 4)), dma((2, 4)),
            dma((8,)), dma((8,)),
            dma((2, 2, 7)), dma((2, 2, 7)),
            dma((2, 8)), dma((2, 8)),
            dma((4, 2)), dma((2,)), dma((4,)), dma((2, 2)),
        ]
        return pl.pallas_call(
            functools.partial(layer_kernel, group),
            out_shape=jax.ShapeDtypeStruct((tokens, dim), BF16),
            in_specs=[pl.BlockSpec(memory_space=pl.ANY)] * 6,
            out_specs=pl.BlockSpec(memory_space=pl.ANY),
            scratch_shapes=scratch,
            compiler_params=pltpu.CompilerParams(collective_id=0, has_side_effects=True,
                                                 vmem_limit_bytes=67043328),
            name='moe_layer',
        )(expert_ids, router_w, act_in, w_gate, w_up, w_down)

    row_spec = P(('dp', 'ep'), None)
    expert_spec = P('ep', None, None)
    return jax.shard_map(device_fn, mesh=mesh,
                         in_specs=(row_spec, P(None, None), row_spec, expert_spec, expert_spec, expert_spec),
                         out_specs=row_spec, check_vma=False)
```

```python
import functools

import jax
import jax.numpy as jnp
from jax import lax
from jax.experimental import pallas as pl
from jax.experimental.pallas import tpu as pltpu
from jax.sharding import PartitionSpec as P

MESH = pl.DeviceIdType.MESH
F32 = jnp.float32
BF16 = jnp.bfloat16

POS = {4: 0, -4: 0, 0: 1, -3: 2, 3: 3, -2: 4, 2: 5, -1: 6, 1: 7}
SIGN = (1, -1)
BACK = ((4, 0), (3, 1), (3, 0), (2, 1), (2, 0), (1, 1), (1, 0))
GU_TILE = 512
DN_TILE = 2048
PIECES = 4


def dot(a, b):
    return jnp.dot(a, b, preferred_element_type=F32)


def layer_kernel(group, ids_hbm, rw_hbm, x_hbm, wg_hbm, wu_hbm, wd_hbm, out_hbm,
                 xg, meta, ids_v, rw_v, tp, xe, hid, eo, cm, part, sib, inb, outv, wgu, wdn,
                 ag_s, ag_r, dx_s, dx_r, mt_s, mt_r, dm_s, dm_r, rs_s, rs_r, sb_s, sb_r,
                 gu_sem, dn_sem, ld_sem, st_sem):
    micro = 64
    half = 32
    piece_rows = micro // PIECES
    me = lax.axis_index('ep')
    core = lax.rem(me, 2)
    other = 1 - core
    nbr = (lax.rem(me + 2, group), lax.rem(me + group - 2, group))
    sibling = me + 1 - 2 * core
    local_experts = wg_hbm.shape[0]
    slots = xe.shape[1] // 4

    def remote(src, dst, ssem, rsem, dev):
        return pltpu.make_async_remote_copy(src_ref=src, dst_ref=dst, send_sem=ssem, recv_sem=rsem,
                                            device_id={'ep': dev}, device_id_type=MESH)

    def gu_copies(e, f):
        cols = pl.ds(f * GU_TILE, GU_TILE)
        return (pltpu.make_async_copy(wg_hbm.at[e, :, cols], wgu.at[f, 0], gu_sem.at[f]),
                pltpu.make_async_copy(wu_hbm.at[e, :, cols], wgu.at[f, 1], gu_sem.at[f]))

    def dn_copy(e, n):
        return pltpu.make_async_copy(wd_hbm.at[e, :, pl.ds(n * DN_TILE, DN_TILE)], wdn.at[n], dn_sem.at[n])

    def x_rows(m, pos, c, start, size):
        row = pl.multiple_of((pos % 2) * 2 * micro + c * micro + start, 16)
        return xg.at[m, pos // 2, pl.ds(row, size)]

    def ag_copy(m, d, k, i):
        start = ((i + d * PIECES // 2) % PIECES) * piece_rows
        src = x_rows(m, POS[-SIGN[d] * k], core, start, piece_rows)
        dst = x_rows(m, POS[-SIGN[d] * (k + 1)], core, start, piece_rows)
        return remote(src, dst, ag_s.at[m, d], ag_r.at[d, k, i], nbr[d])

    def ag_has(k, i):
        return k < 3 or i < PIECES // 2

    def landed(ref, sem):
        pltpu.make_async_copy(ref, ref, sem).wait()

    def dx_copy(m, pos, c):
        ref = x_rows(m, pos, c, 0, micro)
        return remote(ref, ref, dx_s.at[m], dx_r.at[m, pos // 2], sibling)

    def mt_copy(d, k):
        return remote(meta.at[POS[-SIGN[d] * k], core], meta.at[POS[-SIGN[d] * (k + 1)], core],
                      mt_s, mt_r.at[d, k], nbr[d])

    def mt_has(d, k):
        return k < 3 or d == 0

    def dm_copy(pos, c):
        return remote(meta.at[pos, c], meta.at[pos, c], dm_s, dm_r.at[pos // 2], sibling)

    def send_own(m, first, last):
        for i in range(first, last):
            for d in range(2):
                ag_copy(m, d, 0, i).start()
        if last == PIECES:
            dx_copy(m, POS[0], core).start()

    def ag_event(m, k, i):
        for d in range(2):
            ag_copy(m, d, k, i).wait_recv()
            if k < 3 and ag_has(k + 1, i):
                ag_copy(m, d, k + 1, i).start()
        if not ag_has(k, i + 1) or i + 1 == PIECES:
            for pos in ((POS[4],) if k == 3 else (POS[-(k + 1)], POS[k + 1])):
                dx_copy(m, pos, core).start()

    def mt_event(k):
        for d in range(2):
            if mt_has(d, k):
                mt_copy(d, k).wait_recv()
                if k < 3 and mt_has(d, k + 1):
                    mt_copy(d, k + 1).start()
                dm_copy(POS[-SIGN[d] * (k + 1)], core).start()

    def make_meta():
        for m in range(2):
            rows = x_rows(m, POS[0], core, 0, micro)
            tp[m * micro:(m + 1) * micro, 0:rw_v.shape[0]] = lax.dot_general(
                rows[...], rw_v[...], (((1,), (1,)), ((), ())), preferred_element_type=F32)
        ids = ids_v[...].astype(F32)
        expert = lax.broadcasted_iota(jnp.int32, (rw_v.shape[0], 2 * micro), 0).astype(F32)
        logits = tp[...].T[0:rw_v.shape[0]]
        picked = []
        for j in range(8):
            picked.append(jnp.sum(jnp.where(expert == ids[j:j + 1], logits, 0.0), axis=0, keepdims=True))
        picked = jnp.concatenate(picked, axis=0)
        top = jnp.exp(picked - jnp.max(picked, axis=0, keepdims=True))
        gates = top / jnp.sum(top, axis=0, keepdims=True)
        both = jnp.concatenate([ids, gates], axis=0)
        turned = pltpu.roll(both, micro, 1)
        mine = lax.broadcasted_iota(jnp.int32, both.shape, 1) // micro == core
        for m in range(2):
            meta[POS[0], core, m] = jnp.where(mine, jnp.where(core == m, both, turned), 0.0)

    def gather(m, p):
        token = 4 * micro
        info = jnp.concatenate([meta[2 * p, 0, m] + meta[2 * p, 1, m],
                                meta[2 * p + 1, 0, m] + meta[2 * p + 1, 1, m]], axis=1)
        ids, gates = info[0:8], info[8:16]
        chosen, weight = [], []
        for e in range(local_experts):
            hit = ids == (me * local_experts + e).astype(F32)
            chosen.append(jnp.sum(jnp.where(hit, 1.0, 0.0), axis=0, keepdims=True))
            weight.append(jnp.sum(jnp.where(hit, gates, 0.0), axis=0, keepdims=True))
        stacked = jnp.concatenate(chosen + [jnp.zeros((16 - local_experts, token), F32)], axis=0)
        row = lax.broadcasted_iota(jnp.int32, (token, token), 0)
        col = lax.broadcasted_iota(jnp.int32, (token, token), 1)
        before = jnp.where(row < col, 1.0, 0.0).astype(BF16)
        eye = jnp.where(row == col, 1.0, 0.0).astype(BF16)
        rank = dot(stacked.astype(BF16), before)
        slot = lax.broadcasted_iota(jnp.int32, (slots, token), 0).astype(F32)
        pick, mix = [], []
        for e in range(local_experts):
            place = jnp.where(chosen[e] > 0.5, rank[e:e + 1], -1.0)
            at = slot == place
            pick.append(jnp.where(at, 1.0, 0.0))
            mix.append(jnp.where(at, weight[e], 0.0))
        pick = jnp.concatenate(pick, axis=0).astype(BF16)
        rest = jnp.concatenate(mix, axis=0)
        terms = []
        for i in range(3):
            terms.append(rest.astype(BF16))
            rest = rest - terms[i].astype(F32)
        terms = jnp.concatenate(terms, axis=0)
        cm[p] = lax.dot_general(eye, terms, (((1,), (1,)), ((), ())), preferred_element_type=F32).astype(BF16)
        for n in range(0, xg.shape[-1], 512):
            rows = dot(pick, xg[m, p, :, n:n + 512]).astype(BF16)
            for e in range(local_experts):
                xe[e, pl.ds(pl.multiple_of(p * slots, 16), slots), n:n + 512] = rows[e * slots:(e + 1) * slots]

    def experts(first, last, service):
        @pl.loop(first, last)
        def _(e):
            nxt = lax.rem(e + 1, local_experts)

            def after(step):
                for at, fn in service.items():
                    if at[1] == step:
                        pl.when(e == at[0])(fn)

            for f in range(2):
                landed(wgu.at[f], gu_sem.at[f])
                for c in range(0, GU_TILE, 256):
                    a = dot(xe[e], wgu[f, 0, :, c:c + 256])
                    b = dot(xe[e], wgu[f, 1, :, c:c + 256])
                    hid[:, f * GU_TILE + c:f * GU_TILE + c + 256] = (a * jax.nn.sigmoid(a) * b).astype(BF16)
                for cp in gu_copies(nxt, f):
                    cp.start()
                after(f)
            dn_copy(e, 0).wait()
            for c in range(0, DN_TILE, 256):
                o = dot(hid[...], wdn[0, :, c:c + 256]).astype(BF16)
                for p in range(4):
                    eo[p, pl.ds(pl.multiple_of(e * slots, 16), slots), c:c + 256] = o[p * slots:(p + 1) * slots]
            dn_copy(nxt, 0).start()
            after(2)

    def combine(pos):
        p, top = pos // 2, (pos % 2) * 2 * micro
        if not isinstance(pos, int):
            top = pl.multiple_of(top, 2 * micro)
        gates = cm[p, pl.ds(top, 2 * micro)]
        for n in range(0, xg.shape[-1], 512):
            o = eo[p, :, n:n + 512]
            acc = dot(gates, jnp.concatenate([o, o, o], axis=0))
            part[pos, 0, :, n:n + 512] = acc[:micro]
            part[pos, 1, :, n:n + 512] = acc[micro:]

    def sb_copy(m, pos):
        return remote(part.at[pos, other], sib.at[m, pos], sb_s.at[pos], sb_r.at[m, pos], sibling)

    def back_item(d, j):
        dist, rows = BACK[j]
        return POS[SIGN[d] * dist], (rows if d == 0 else 1 - rows)

    def rs_copy(m, d, j):
        pos, r = back_item(d, j)
        return remote(part.at[pos, core, pl.ds(r * half, half)], inb.at[d, j],
                      rs_s.at[pos], rs_r.at[d, j], nbr[d])

    here = set()

    def need_sib(m, pos):
        if (m, pos) not in here:
            here.add((m, pos))
            sb_copy(m, pos).wait_recv()

    def back(m, j):
        for d in range(2):
            pos, r = back_item(d, j)
            need_sib(m, pos)
            rows = pl.ds(r * half, half)
            acc = part[pos, core, rows] + sib[m, pos, rows]
            if j >= 2:
                rs_copy(m, d, j - 2).wait_recv()
                acc = acc + inb[d, j - 2]
            part[pos, core, rows] = acc
            rs_copy(m, d, j).start()

    def st_copy(m, r):
        rows = pl.ds(m * micro + r * half, half)
        return pltpu.make_async_copy(outv.at[rows], out_hbm.at[rows], st_sem)

    def finish(m, r):
        pos = POS[0]
        need_sib(m, pos)
        rows = pl.ds(r * half, half)
        acc = part[pos, core, rows] + sib[m, pos, rows]
        for d in range(2):
            j = 5 if (r == 1) == (d == 0) else 6
            if (m, d, j) not in here:
                here.add((m, d, j))
                rs_copy(m, d, j).wait_recv()
            acc = acc + inb[d, j]
        outv[pl.ds(m * micro + r * half, half)] = acc.astype(BF16)
        st_copy(m, r).start()

    def combine_send(m, pos):
        combine(pos)
        sb_copy(m, pos).start()

    def combine_loop(m, first, last):
        @pl.loop(first, last)
        def _(pos):
            combine_send(m, pos)

    def part_free(m, pos):
        landed(part.at[pos, other], sb_s.at[pos])
        if pos != POS[0]:
            landed(part.at[pos, core], rs_s.at[pos])

    def pair_wait(m, p):
        landed(xg.at[m, p, pl.ds(0, 2 * micro)], dx_r.at[m, p])
        if m == 0:
            landed(meta.at[pl.ds(2 * p, 2), 0], dm_r.at[p])

    loads = [pltpu.make_async_copy(x_hbm.at[pl.ds(m * micro, micro)], x_rows(m, POS[0], core, 0, micro), ld_sem.at[m])
             for m in range(2)]
    loads.append(pltpu.make_async_copy(ids_hbm, ids_v, ld_sem.at[2]))
    loads.append(pltpu.make_async_copy(rw_hbm, rw_v, ld_sem.at[3]))
    for cp in loads:
        cp.start()

    def enter():
        barrier = pltpu.get_barrier_semaphore()
        for dev in (nbr[0], nbr[1], sibling):
            pl.semaphore_signal(barrier, inc=1, device_id={'ep': dev}, device_id_type=MESH)
        pl.semaphore_wait(barrier, 3)

    enter()
    loads[0].wait()

    send_own(0, 0, PIECES // 2)
    for cp in loads[2:]:
        cp.wait()
    loads[1].wait()
    make_meta()
    for d in range(2):
        mt_copy(d, 0).start()
    dm_copy(POS[0], core).start()
    send_own(0, PIECES // 2, PIECES)
    for f in range(2):
        for cp in gu_copies(0, f):
            cp.start()
    dn_copy(0, 0).start()

    for k in range(3):
        for i in range(PIECES):
            ag_event(0, k, i)
            if i == 1:
                mt_event(k)
                if k == 2:
                    send_own(1, 0, PIECES)
        if k == 1:
            pair_wait(0, 3)
            gather(0, 3)
    pair_wait(0, 2)
    gather(0, 2)
    ag_event(0, 3, 0)
    ag_event(0, 3, 1)
    mt_event(3)
    pair_wait(0, 1)
    gather(0, 1)
    pair_wait(0, 0)
    gather(0, 0)

    experts(0, local_experts, {
        (0, 0): lambda: ag_event(1, 0, 0),
        (0, 1): lambda: ag_event(1, 0, 1),
        (0, 2): lambda: ag_event(1, 0, 2),
        (1, 1): lambda: ag_event(1, 0, 3),
        (1, 2): lambda: ag_event(1, 1, 0),
        (2, 0): lambda: ag_event(1, 1, 1),
        (2, 2): lambda: ag_event(1, 1, 2),
        (3, 0): lambda: ag_event(1, 1, 3),
        (3, 2): lambda: ag_event(1, 2, 0),
    })
    combine_send(0, 0)
    ag_event(1, 2, 1)
    combine_loop(0, 2, 4)
    ag_event(1, 2, 2)
    ag_event(1, 2, 3)
    back(0, 0)
    back(0, 1)
    combine_loop(0, 4, 8)
    combine_send(0, 1)
    ag_event(1, 3, 0)
    ag_event(1, 3, 1)
    for p in range(4):
        pair_wait(1, p)

    @pl.loop(0, 4)
    def _(p):
        gather(1, p)

    for j in range(2, 7):
        for d in range(2):
            need_sib(0, back_item(d, j)[0])

    experts(0, local_experts, {
        (1, 0): lambda: back(0, 2),
        (2, 2): lambda: back(0, 3),
    })
    back(0, 4)
    part_free(0, 0)
    combine_send(1, 0)
    part_free(0, 2)
    part_free(0, 3)
    combine_loop(1, 2, 4)
    back(0, 5)
    back(0, 6)
    back(1, 0)
    back(1, 1)
    finish(0, 0)
    finish(0, 1)
    for pos in (4, 5, 6, 7, 1):
        part_free(0, pos)
    combine_loop(1, 4, 8)
    combine_send(1, 1)
    for j in range(2, 7):
        back(1, j)
    finish(1, 0)
    finish(1, 1)

    def drain():
        for m in range(2):
            for d in range(2):
                landed(xg.at[m, 0, pl.ds(0, (3 * PIECES + PIECES // 2) * piece_rows)], ag_s.at[m, d])
            landed(xg.at[m, pl.ds(0, 2)], dx_s.at[m])
        landed(meta.at[pl.ds(0, 7), 0], mt_s)
        landed(meta.at[pl.ds(0, 8), 0], dm_s)
        for pos in range(8):
            part_free(1, pos)
        for f in range(2):
            landed(wgu.at[f], gu_sem.at[f])
        dn_copy(0, 0).wait()
        landed(outv, st_sem)

    drain()


def solution(mesh):
    group = mesh.shape['ep']

    def device_fn(act_in, router_w, expert_ids, w_gate, w_up, w_down):
        tokens, dim = act_in.shape
        local_experts, _, ffn = w_gate.shape
        micro = tokens // 2
        half = micro // 2
        mean_load = micro * expert_ids.shape[1] // (local_experts * group)
        cap = mean_load + mean_load // 2
        slots = 4 * cap
        dma = pltpu.SemaphoreType.DMA
        scratch = [
            pltpu.VMEM((2, 4, 4 * micro, dim), BF16),
            pltpu.VMEM((8, 2, 2, 16, 2 * micro), F32),
            pltpu.VMEM(expert_ids.shape[::-1], jnp.int32),
            pltpu.VMEM(router_w.shape[::-1], BF16),
            pltpu.VMEM((tokens, 128), F32),
            pltpu.VMEM((local_experts, 4 * slots, dim), BF16),
            pltpu.VMEM((4 * slots, ffn), BF16),
            pltpu.VMEM((4, local_experts * slots, dim), BF16),
            pltpu.VMEM((4, 4 * micro, 3 * local_experts * slots), BF16),
            pltpu.VMEM((8, 2, micro, dim), F32),
            pltpu.VMEM((2, 8, micro, dim), F32),
            pltpu.VMEM((2, 7, half, dim), F32),
            pltpu.VMEM((tokens, dim), BF16),
            pltpu.VMEM((2, 2, dim, GU_TILE), BF16),
            pltpu.VMEM((1, ffn, DN_TILE), BF16),
            dma((2, 2)), dma((2, 4, PIECES)),
            dma((2,)), dma((2, 4)),
            dma, dma((2, 4)),
            dma, dma((4,)),
            dma((8,)), dma((2, 7)),
            dma((8,)), dma((2, 8)),
            dma((2,)), dma((1,)), dma((4,)), dma,
        ]
        return pl.pallas_call(
            functools.partial(layer_kernel, group),
            out_shape=jax.ShapeDtypeStruct((tokens, dim), BF16),
            in_specs=[pl.BlockSpec(memory_space=pl.ANY)] * 6,
            out_specs=pl.BlockSpec(memory_space=pl.ANY),
            scratch_shapes=scratch,
            compiler_params=pltpu.CompilerParams(collective_id=0, has_side_effects=True,
                                                 vmem_limit_bytes=67043328),
            name='moe_layer',
        )(expert_ids.T, router_w.T, act_in, w_gate, w_up, w_down)

    row_spec = P(('dp', 'ep'), None)
    expert_spec = P('ep', None, None)
    return jax.shard_map(device_fn, mesh=mesh,
                         in_specs=(row_spec, P(None, None), row_spec, expert_spec, expert_spec, expert_spec),
                         out_specs=row_spec, check_vma=False)
```

```python
import functools

import jax
import jax.numpy as jnp
from jax import lax
from jax.experimental import pallas as pl
from jax.experimental.pallas import tpu as pltpu
from jax.sharding import PartitionSpec as P

MESH = pl.DeviceIdType.MESH
F32 = jnp.float32
BF16 = jnp.bfloat16

FAR = 4
ORDER = (FAR, 0, -3, 3, -2, 2, -1, 1)
POS = {away: i for i, away in enumerate(ORDER)}
POS[-FAR] = POS[FAR]
HERE = POS[0]
CHIPS = len(ORDER)
PAIRS = CHIPS // 2
SIGN = (1, -1)
TERMS = 3
NT = (((1,), (1,)), ((), ()))
BACK = ((FAR, 0),) + tuple((away, r) for away in range(FAR - 1, 0, -1) for r in (1, 0))
SENDS = len(BACK)
STEPS = 3
GU_TILE = 512
WIDE = 512
MXU = 256
PIECES = 4


def dot(a, b):
    return jnp.dot(a, b, preferred_element_type=F32)


def layer_kernel(group, ids_hbm, rw_hbm, x_hbm, wg_hbm, wu_hbm, wd_hbm, out_hbm,
                 xg, meta, ids_v, rw_v, tp, xe, hid, eo, picks, cm, part, sib, inb, outv, wgu, wdn,
                 ag_s, ag_r, dx_s, dx_r, mt_s, mt_r, dm_s, dm_r, rs_s, rs_r, sb_s, sb_r,
                 gu_sem, dn_sem, ld_sem, st_sem):
    micro = outv.shape[0] // 2
    chip = 2 * micro
    half = micro // 2
    dim = outv.shape[1]
    last = FAR - 1
    piece_rows = micro // PIECES
    me = lax.axis_index('ep')
    core = lax.rem(me, 2)
    other = 1 - core
    nbr = (lax.rem(me + 2, group), lax.rem(me + group - 2, group))
    sibling = me + 1 - 2 * core
    local_experts = wg_hbm.shape[0]
    slots = xe.shape[1] // 4

    def remote(src, dst, ssem, rsem, dev):
        return pltpu.make_async_remote_copy(src_ref=src, dst_ref=dst, send_sem=ssem, recv_sem=rsem,
                                            device_id={'ep': dev}, device_id_type=MESH)

    def gu_copies(e, f):
        cols = pl.ds(f * GU_TILE, GU_TILE)
        s = lax.rem(e, 2)
        return (pltpu.make_async_copy(wg_hbm.at[e, :, cols], wgu.at[s, f, 0], gu_sem.at[s, f]),
                pltpu.make_async_copy(wu_hbm.at[e, :, cols], wgu.at[s, f, 1], gu_sem.at[s, f]))

    def dn_copy(e):
        return pltpu.make_async_copy(wd_hbm.at[e], wdn.at[lax.rem(e, 2)], dn_sem.at[lax.rem(e, 2)])

    def load_weights():
        for e in range(2):
            for f in range(2):
                for cp in gu_copies(e, f):
                    cp.start()
            dn_copy(e).start()

    def x_rows(m, pos, c, start, size):
        row = pl.multiple_of((pos % 2) * chip + c * micro + start, 16)
        return xg.at[m, pos // 2, pl.ds(row, size)]

    def ag_copy(m, d, k, i):
        start = ((i + d * PIECES // 2) % PIECES) * piece_rows
        src = x_rows(m, POS[-SIGN[d] * k], core, start, piece_rows)
        dst = x_rows(m, POS[-SIGN[d] * (k + 1)], core, start, piece_rows)
        return remote(src, dst, ag_s.at[m, d], ag_r.at[d, k, i], nbr[d])

    def ag_has(k, i):
        return k < last or i < PIECES // 2

    def landed(ref, sem):
        pltpu.make_async_copy(ref, ref, sem).wait()

    def dx_copy(m, pos, c):
        ref = x_rows(m, pos, c, 0, micro)
        return remote(ref, ref, dx_s.at[m], dx_r.at[m, pos // 2], sibling)

    def mt_copy(d, k):
        return remote(meta.at[POS[-SIGN[d] * k], core], meta.at[POS[-SIGN[d] * (k + 1)], core],
                      mt_s, mt_r.at[d, k], nbr[d])

    def mt_has(d, k):
        return k < last or d == 0

    def dm_copy(pos, c):
        return remote(meta.at[pos, c], meta.at[pos, c], dm_s, dm_r.at[pos // 2], sibling)

    def send_own(m, first, last):
        for i in range(first, last):
            for d in range(2):
                ag_copy(m, d, 0, i).start()
        if last == PIECES:
            dx_copy(m, HERE, core).start()

    def ag_event(m, k, i):
        for d in range(2):
            ag_copy(m, d, k, i).wait_recv()
            if k < last and ag_has(k + 1, i):
                ag_copy(m, d, k + 1, i).start()
        if k == last:
            for d in range(2):
                ref = x_rows(m, POS[FAR], core, (i + d * PIECES // 2) * piece_rows, piece_rows)
                remote(ref, ref, dx_s.at[m], dx_r.at[m, POS[FAR] // 2], sibling).start()
        elif i + 1 == PIECES:
            for d in range(2):
                dx_copy(m, POS[-SIGN[d] * (k + 1)], core).start()

    def take(m, first, after):
        for n in range(first, after):
            ag_event(m, n // PIECES, n % PIECES)

    def mt_event(k):
        for d in range(2):
            if mt_has(d, k):
                mt_copy(d, k).wait_recv()
                if k < last and mt_has(d, k + 1):
                    mt_copy(d, k + 1).start()
                dm_copy(POS[-SIGN[d] * (k + 1)], core).start()

    def make_meta():
        for m in range(2):
            rows = x_rows(m, HERE, core, 0, micro)
            tp[m * micro:(m + 1) * micro, 0:rw_v.shape[0]] = lax.dot_general(
                rows[...], rw_v[...], NT, preferred_element_type=F32)
        ids = ids_v[...].astype(F32)
        expert = lax.broadcasted_iota(jnp.int32, (rw_v.shape[0], chip), 0).astype(F32)
        logits = tp[...].T[0:rw_v.shape[0]]
        picked = []
        for j in range(8):
            picked.append(jnp.sum(jnp.where(expert == ids[j:j + 1], logits, 0.0), axis=0, keepdims=True))
        picked = jnp.concatenate(picked, axis=0)
        top = jnp.exp(picked - jnp.max(picked, axis=0, keepdims=True))
        gates = top / jnp.sum(top, axis=0, keepdims=True)
        both = jnp.concatenate([ids, gates], axis=0)
        turned = pltpu.roll(both, micro, 1)
        mine = lax.broadcasted_iota(jnp.int32, both.shape, 1) // micro == core
        for m in range(2):
            meta[HERE, core, m] = jnp.where(mine, jnp.where(core == m, both, turned), 0.0)

    def index(m, p):
        token = 2 * chip
        info = jnp.concatenate([meta[2 * p, 0, m] + meta[2 * p, 1, m],
                                meta[2 * p + 1, 0, m] + meta[2 * p + 1, 1, m]], axis=1)
        ids, gates = info[0:8], info[8:16]
        chosen, weight = [], []
        for e in range(local_experts):
            hit = ids == (me * local_experts + e).astype(F32)
            chosen.append(jnp.sum(jnp.where(hit, 1.0, 0.0), axis=0, keepdims=True))
            weight.append(jnp.sum(jnp.where(hit, gates, 0.0), axis=0, keepdims=True))
        stacked = jnp.concatenate(chosen + [jnp.zeros((16 - local_experts, token), F32)], axis=0)
        row = lax.broadcasted_iota(jnp.int32, (token, token), 0)
        col = lax.broadcasted_iota(jnp.int32, (token, token), 1)
        before = jnp.where(row < col, 1.0, 0.0).astype(BF16)
        eye = jnp.where(row == col, 1.0, 0.0).astype(BF16)
        rank = dot(stacked.astype(BF16), before)
        slot = lax.broadcasted_iota(jnp.int32, (slots, token), 0).astype(F32)
        pick, mix = [], []
        for e in range(local_experts):
            place = jnp.where(chosen[e] > 0.5, rank[e:e + 1], -1.0)
            at = slot == place
            pick.append(jnp.where(at, 1.0, 0.0))
            mix.append(jnp.where(at, weight[e], 0.0))
        picks[m, p] = jnp.concatenate(pick, axis=0).astype(BF16)
        rest = jnp.concatenate(mix, axis=0)
        terms = []
        for i in range(TERMS):
            terms.append(rest.astype(BF16))
            rest = rest - terms[i].astype(F32)
        terms = jnp.concatenate(terms, axis=0)
        cm[m, p] = lax.dot_general(eye, terms, NT, preferred_element_type=F32).astype(BF16)

    def gather(m, p):
        for n in range(0, dim, WIDE):
            rows = dot(picks[m, p], xg[m, p, :, n:n + WIDE]).astype(BF16)
            for e in range(local_experts):
                xe[e, pl.ds(pl.multiple_of(p * slots, 16), slots), n:n + WIDE] = rows[e * slots:(e + 1) * slots]

    def experts(m, service):
        @pl.loop(0, local_experts)
        def _(e):
            s = lax.rem(e, 2)
            nxt = lax.rem(e + 2, local_experts)

            def after(step, copies):
                def start():
                    for cp in copies:
                        cp.start()

                if m == 0:
                    start()
                else:
                    pl.when(e + 2 < local_experts)(start)
                for at, fn in service.items():
                    if at[1] == step:
                        who = functools.reduce(lambda x, c: x & (core == c), at[2:], e == at[0])
                        pl.when(who)(fn)

            for f in range(2):
                landed(wgu.at[s, f], gu_sem.at[s, f])
                for c in range(0, GU_TILE, MXU):
                    a = dot(xe[e], wgu[s, f, 0, :, c:c + MXU])
                    b = dot(xe[e], wgu[s, f, 1, :, c:c + MXU])
                    hid[:, f * GU_TILE + c:f * GU_TILE + c + MXU] = (a * jax.nn.sigmoid(a) * b).astype(BF16)
                after(f, gu_copies(nxt, f))
            dn_copy(e).wait()
            for c in range(0, dim, MXU):
                o = dot(hid[...], wdn[s, :, c:c + MXU]).astype(BF16)
                for p in range(4):
                    eo[p, pl.ds(pl.multiple_of(e * slots, 16), slots), c:c + MXU] = o[p * slots:(p + 1) * slots]
            after(2, (dn_copy(nxt),))

    def combine(m, pos):
        p, top = pos // 2, (pos % 2) * chip
        if not isinstance(pos, int):
            top = pl.multiple_of(top, chip)
        gates = cm[m, p, pl.ds(top, chip)]
        for n in range(0, dim, WIDE):
            o = eo[p, :, n:n + WIDE]
            acc = dot(gates, jnp.concatenate([o, o, o], axis=0))
            part[pos, 0, :, n:n + WIDE] = acc[:micro]
            part[pos, 1, :, n:n + WIDE] = acc[micro:]

    def sb_copy(m, pos):
        return remote(part.at[pos, other], sib.at[m, pos], sb_s.at[pos], sb_r.at[m, pos], sibling)

    def back_item(d, j):
        dist, rows = BACK[j]
        return POS[SIGN[d] * dist], (rows if d == 0 else 1 - rows)

    def rs_copy(m, d, j):
        pos, r = back_item(d, j)
        return remote(part.at[pos, core, pl.ds(r * half, half)], inb.at[d, j],
                      rs_s.at[pos], rs_r.at[d, j], nbr[d])

    seen = set()

    def need_sib(m, pos):
        if (m, pos) not in seen:
            seen.add((m, pos))
            sb_copy(m, pos).wait_recv()

    def back(m, j):
        for d in range(2):
            pos, r = back_item(d, j)
            need_sib(m, pos)
            rows = pl.ds(r * half, half)
            acc = part[pos, core, rows] + sib[m, pos, rows]
            if j >= 2:
                rs_copy(m, d, j - 2).wait_recv()
                acc = acc + inb[d, j - 2]
            part[pos, core, rows] = acc
            rs_copy(m, d, j).start()

    def st_copy(m, r):
        rows = pl.ds(m * micro + r * half, half)
        return pltpu.make_async_copy(outv.at[rows], out_hbm.at[rows], st_sem)

    def finish(m, r):
        pos = HERE
        need_sib(m, pos)
        rows = pl.ds(r * half, half)
        acc = part[pos, core, rows] + sib[m, pos, rows]
        for d in range(2):
            j = 5 if (r == 1) == (d == 0) else 6
            if (m, d, j) not in seen:
                seen.add((m, d, j))
                rs_copy(m, d, j).wait_recv()
            acc = acc + inb[d, j]
        outv[pl.ds(m * micro + r * half, half)] = acc.astype(BF16)
        st_copy(m, r).start()

    def combine_send(m, pos):
        combine(m, pos)
        sb_copy(m, pos).start()

    def combine_loop(m, first, last):
        @pl.loop(first, last)
        def _(pos):
            combine_send(m, pos)

    def part_free(m, pos):
        landed(part.at[pos, other], sb_s.at[pos])
        if pos != HERE:
            landed(part.at[pos, core], rs_s.at[pos])

    def pair_wait(m, p):
        landed(xg.at[m, p, pl.ds(0, chip)], dx_r.at[m, p])

    def info_wait(p):
        landed(meta.at[pl.ds(2 * p, 2), 0], dm_r.at[p])

    loads = [pltpu.make_async_copy(x_hbm.at[pl.ds(m * micro, micro)], x_rows(m, HERE, core, 0, micro), ld_sem.at[m])
             for m in range(2)]
    loads.append(pltpu.make_async_copy(ids_hbm, ids_v, ld_sem.at[2]))
    loads.append(pltpu.make_async_copy(rw_hbm, rw_v, ld_sem.at[3]))
    for cp in loads:
        cp.start()

    def enter():
        barrier = pltpu.get_barrier_semaphore()
        for dev in (nbr[0], nbr[1], sibling):
            pl.semaphore_signal(barrier, inc=1, device_id={'ep': dev}, device_id_type=MESH)
        pl.semaphore_wait(barrier, 3)

    enter()
    loads[0].wait()

    send_own(0, 0, 1)
    for cp in loads[2:]:
        cp.wait()
    loads[1].wait()
    make_meta()
    for d in range(2):
        mt_copy(d, 0).start()
    dm_copy(HERE, core).start()
    send_own(0, 1, PIECES)
    load_weights()

    def prepare(p):
        info_wait(p)
        index(0, p)

    def fetch(m, p):
        pair_wait(m, p)
        gather(m, p)

    near, mid, wide, far = 3, 2, 1, 0
    for k in range(last - 1):
        mt_event(k)
        take(0, k * PIECES, (k + 1) * PIECES)
    prepare(near)
    pair_wait(0, near)
    mt_event(last - 1)
    n = (last - 1) * PIECES
    take(0, n, n + 1)
    gather(0, near)
    take(0, n + 1, n + 2)
    send_own(1, 0, PIECES)
    index(1, near)
    take(0, n + 2, n + 3)
    prepare(mid)
    take(0, n + 3, n + PIECES)
    fetch(0, mid)
    n = last * PIECES
    mt_event(last)
    prepare(wide)
    take(0, n, n + 1)
    prepare(far)
    take(0, n + 1, n + 2)
    pl.when(core == 1)(functools.partial(take, 1, 0, 1))
    fetch(0, wide)
    fetch(0, far)
    pl.when(core == 1)(functools.partial(take, 1, 1, 2))

    due = {}
    for c, first, steps in ((0, 0, (0, 1, 3, 4, 6, 7, 9, 10, 11)), (1, 2, (0, 2, 3, 4, 6, 7, 8, 10))):
        for n, step in enumerate(steps, first):
            due[divmod(step, STEPS) + (c,)] = functools.partial(take, 1, n, n + 1)
    experts(0, due)
    combine_send(0, 0)
    n = (last - 1) * PIECES + 1
    pl.when(core == 0)(functools.partial(take, 1, n, n + 1))
    combine_loop(0, 2, FAR)
    back(0, 0)
    take(1, n + 1, last * PIECES)
    back(0, 1)
    combine_loop(0, FAR, FAR + 2)
    take(1, last * PIECES, last * PIECES + 2)
    combine_loop(0, FAR + 2, CHIPS)
    combine_send(0, HERE)
    for p in range(near):
        index(1, p)
    for p in range(PAIRS):
        fetch(1, p)

    for j in range(2, SENDS):
        for d in range(2):
            need_sib(0, back_item(d, j)[0])

    experts(1, {
        (0, 2): functools.partial(back, 0, 2),
        (2, 2): functools.partial(back, 0, 3),
    })
    part_free(0, 0)
    combine_send(1, 0)
    back(0, 4)
    part_free(0, 2)
    part_free(0, 3)
    combine_loop(1, 2, FAR)
    back(0, 5)
    back(0, 6)
    back(1, 0)
    back(1, 1)
    finish(0, 0)
    finish(0, 1)
    for pos in (HERE, *range(FAR, CHIPS)):
        part_free(0, pos)
    combine_loop(1, FAR, CHIPS)
    combine_send(1, HERE)
    for j in range(2, SENDS):
        back(1, j)
    finish(1, 0)
    finish(1, 1)

    def drain():
        for m in range(2):
            for d in range(2):
                landed(xg.at[m, 0, pl.ds(0, (3 * PIECES + PIECES // 2) * piece_rows)], ag_s.at[m, d])
            landed(xg.at[m, pl.ds(0, 2)], dx_s.at[m])
        landed(meta.at[pl.ds(0, 7), 0], mt_s)
        landed(meta.at[pl.ds(0, 8), 0], dm_s)
        for pos in range(CHIPS):
            part_free(1, pos)
        landed(outv, st_sem)

    drain()


def solution(mesh):
    group = mesh.shape['ep']

    def device_fn(act_in, router_w, expert_ids, w_gate, w_up, w_down):
        tokens, dim = act_in.shape
        local_experts, _, ffn = w_gate.shape
        micro = tokens // 2
        half = micro // 2
        mean_load = micro * expert_ids.shape[1] // (local_experts * group)
        cap = mean_load + mean_load // 2
        slots = 4 * cap
        dma = pltpu.SemaphoreType.DMA
        scratch = [
            pltpu.VMEM((2, 4, 4 * micro, dim), BF16),
            pltpu.VMEM((8, 2, 2, 16, 2 * micro), F32),
            pltpu.VMEM(expert_ids.shape[::-1], jnp.int32),
            pltpu.VMEM(router_w.shape[::-1], BF16),
            pltpu.VMEM((tokens, 128), F32),
            pltpu.VMEM((local_experts, 4 * slots, dim), BF16),
            pltpu.VMEM((4 * slots, ffn), BF16),
            pltpu.VMEM((4, local_experts * slots, dim), BF16),
            pltpu.VMEM((2, 4, local_experts * slots, 4 * micro), BF16),
            pltpu.VMEM((2, 4, 4 * micro, 3 * local_experts * slots), BF16),
            pltpu.VMEM((8, 2, micro, dim), F32),
            pltpu.VMEM((2, 8, micro, dim), F32),
            pltpu.VMEM((2, 7, half, dim), F32),
            pltpu.VMEM((tokens, dim), BF16),
            pltpu.VMEM((2, 2, 2, dim, GU_TILE), BF16),
            pltpu.VMEM((2, ffn, dim), BF16),
            dma((2, 2)), dma((2, 4, PIECES)),
            dma((2,)), dma((2, 4)),
            dma, dma((2, 4)),
            dma, dma((4,)),
            dma((8,)), dma((2, 7)),
            dma((8,)), dma((2, 8)),
            dma((2, 2)), dma((2,)), dma((4,)), dma,
        ]
        return pl.pallas_call(
            functools.partial(layer_kernel, group),
            out_shape=jax.ShapeDtypeStruct((tokens, dim), BF16),
            in_specs=[pl.BlockSpec(memory_space=pl.ANY)] * 6,
            out_specs=pl.BlockSpec(memory_space=pl.ANY),
            scratch_shapes=scratch,
            compiler_params=pltpu.CompilerParams(collective_id=0, has_side_effects=True,
                                                 vmem_limit_bytes=67043328),
            name='moe_layer',
        )(expert_ids.T, router_w.T, act_in, w_gate, w_up, w_down)

    row_spec = P(('dp', 'ep'), None)
    expert_spec = P('ep', None, None)
    return jax.shard_map(device_fn, mesh=mesh,
                         in_specs=(row_spec, P(None, None), row_spec, expert_spec, expert_spec, expert_spec),
                         out_specs=row_spec, check_vma=False)
```

```python
import functools

import jax
import jax.numpy as jnp
from jax import lax
from jax.experimental import pallas as pl
from jax.experimental.pallas import tpu as pltpu
from jax.sharding import PartitionSpec as P

MESH = pl.DeviceIdType.MESH
F32 = jnp.float32
BF16 = jnp.bfloat16

FAR = 4
ORDER = (FAR, 0, -3, 3, -2, 2, -1, 1)
POS = {away: i for i, away in enumerate(ORDER)}
POS[-FAR] = POS[FAR]
HERE = POS[0]
CHIPS = len(ORDER)
PAIRS = CHIPS // 2
SIGN = (1, -1)
TERMS = 3
NT = (((1,), (1,)), ((), ()))
BACK = ((FAR, 0),) + tuple((away, r) for away in range(FAR - 1, 0, -1) for r in (1, 0))
SENDS = len(BACK)
STEPS = 3
GU_TILE = 512
WIDE = 512
MXU = 256
PIECES = 4


def dot(a, b):
    return jnp.dot(a, b, preferred_element_type=F32)


def layer_kernel(group, ids_hbm, rw_hbm, x_hbm, wg_hbm, wu_hbm, wd_hbm, out_hbm,
                 xg, meta, ids_v, rw_v, tp, xe, hid, eo, picks, cm, fm, rows_out, rows_sib, rows_in, part, sib, inb, outv, wgu, wdn,
                 ag_s, ag_r, dx_s, dx_r, mt_s, mt_r, dm_s, dm_r, rs_s, rs_r, sb_s, sb_r,
                 gu_sem, dn_sem, ld_sem, st_sem):
    micro = outv.shape[0] // 2
    chip = 2 * micro
    dim = outv.shape[1]
    half = dim // 2
    last = FAR - 1
    piece_rows = micro // PIECES
    me = lax.axis_index('ep')
    core = lax.rem(me, 2)
    other = 1 - core
    nbr = (lax.rem(me + 2, group), lax.rem(me + group - 2, group))
    sibling = me + 1 - 2 * core
    local_experts = wg_hbm.shape[0]
    slots = xe.shape[1] // PAIRS
    cap = slots // (2 * 2)

    def remote(src, dst, ssem, rsem, dev):
        return pltpu.make_async_remote_copy(src_ref=src, dst_ref=dst, send_sem=ssem, recv_sem=rsem,
                                            device_id={'ep': dev}, device_id_type=MESH)

    def gu_copies(e, f):
        cols = pl.ds(f * GU_TILE, GU_TILE)
        s = lax.rem(e, 2)
        return (pltpu.make_async_copy(wg_hbm.at[e, :, cols], wgu.at[s, f, 0], gu_sem.at[s, f]),
                pltpu.make_async_copy(wu_hbm.at[e, :, cols], wgu.at[s, f, 1], gu_sem.at[s, f]))

    def dn_copy(e):
        return pltpu.make_async_copy(wd_hbm.at[e], wdn.at[lax.rem(e, 2)], dn_sem.at[lax.rem(e, 2)])

    def load_weights():
        for e in range(2):
            for f in range(2):
                for cp in gu_copies(e, f):
                    cp.start()
            dn_copy(e).start()

    def x_rows(m, pos, c, start, size):
        row = pl.multiple_of((pos % 2) * chip + c * micro + start, 16)
        return xg.at[m, pos // 2, pl.ds(row, size)]

    def ag_copy(m, d, k, i):
        start = ((i + d * PIECES // 2) % PIECES) * piece_rows
        src = x_rows(m, POS[-SIGN[d] * k], core, start, piece_rows)
        dst = x_rows(m, POS[-SIGN[d] * (k + 1)], core, start, piece_rows)
        return remote(src, dst, ag_s.at[m, d], ag_r.at[d, k, i], nbr[d])

    def ag_has(k, i):
        return k < last or i < PIECES // 2

    def landed(ref, sem):
        pltpu.make_async_copy(ref, ref, sem).wait()

    def dx_copy(m, pos, c):
        ref = x_rows(m, pos, c, 0, micro)
        return remote(ref, ref, dx_s.at[m], dx_r.at[m, pos // 2], sibling)

    def mt_copy(d, k):
        return remote(meta.at[POS[-SIGN[d] * k], core], meta.at[POS[-SIGN[d] * (k + 1)], core],
                      mt_s, mt_r.at[d, k], nbr[d])

    def mt_has(d, k):
        return k < last or d == 0

    def dm_copy(pos, c):
        return remote(meta.at[pos, c], meta.at[pos, c], dm_s, dm_r.at[pos // 2], sibling)

    def send_own(m, first, last):
        for i in range(first, last):
            for d in range(2):
                ag_copy(m, d, 0, i).start()
        if last == PIECES:
            dx_copy(m, HERE, core).start()

    def ag_event(m, k, i):
        for d in range(2):
            ag_copy(m, d, k, i).wait_recv()
            if k < last and ag_has(k + 1, i):
                ag_copy(m, d, k + 1, i).start()
        if k == last:
            for d in range(2):
                ref = x_rows(m, POS[FAR], core, (i + d * PIECES // 2) * piece_rows, piece_rows)
                remote(ref, ref, dx_s.at[m], dx_r.at[m, POS[FAR] // 2], sibling).start()
        elif i + 1 == PIECES:
            for d in range(2):
                dx_copy(m, POS[-SIGN[d] * (k + 1)], core).start()

    def take(m, first, after):
        for n in range(first, after):
            ag_event(m, n // PIECES, n % PIECES)

    def mt_event(k):
        for d in range(2):
            if mt_has(d, k):
                mt_copy(d, k).wait_recv()
                if k < last and mt_has(d, k + 1):
                    mt_copy(d, k + 1).start()
                dm_copy(POS[-SIGN[d] * (k + 1)], core).start()

    def make_meta():
        for m in range(2):
            rows = x_rows(m, HERE, core, 0, micro)
            tp[m * micro:(m + 1) * micro, 0:rw_v.shape[0]] = lax.dot_general(
                rows[...], rw_v[...], NT, preferred_element_type=F32)
        ids = ids_v[...].astype(F32)
        expert = lax.broadcasted_iota(jnp.int32, (rw_v.shape[0], chip), 0).astype(F32)
        logits = tp[...].T[0:rw_v.shape[0]]
        picked = []
        for j in range(8):
            picked.append(jnp.sum(jnp.where(expert == ids[j:j + 1], logits, 0.0), axis=0, keepdims=True))
        picked = jnp.concatenate(picked, axis=0)
        top = jnp.exp(picked - jnp.max(picked, axis=0, keepdims=True))
        gates = top / jnp.sum(top, axis=0, keepdims=True)
        both = jnp.concatenate([ids, gates], axis=0)
        turned = pltpu.roll(both, micro, 1)
        mine = lax.broadcasted_iota(jnp.int32, both.shape, 1) // micro == core
        for m in range(2):
            meta[HERE, core, m] = jnp.where(mine, jnp.where(core == m, both, turned), 0.0)

    def grid(shape, axis):
        return lax.broadcasted_iota(jnp.int32, shape, axis)

    def one(mask):
        return jnp.where(mask, 1.0, 0.0).astype(BF16)

    def chip_info(pos, m):
        return meta[pos, 0, m] + meta[pos, 1, m]

    def places(info, first, count):
        token = info.shape[1]
        ids, gates = info[0:8], info[8:16]
        chosen, weight = [], []
        for e in range(count):
            hit = ids == (first + e).astype(F32)
            chosen.append(jnp.sum(jnp.where(hit, 1.0, 0.0), axis=0, keepdims=True))
            weight.append(jnp.sum(jnp.where(hit, gates, 0.0), axis=0, keepdims=True))
        stacked = jnp.concatenate(chosen + [jnp.zeros((info.shape[0] - count, token), F32)], axis=0)
        row, col = grid((token, token), 0), grid((token, token), 1)
        rank = dot(stacked.astype(BF16), one((row < col) & (row // micro == col // micro)))
        return [jnp.where(chosen[e] > 0.5, rank[e:e + 1], -slots) for e in range(count)], weight, one(row == col)

    def three_terms(rest):
        terms = []
        for i in range(TERMS):
            terms.append(rest.astype(BF16))
            rest = rest - terms[i].astype(F32)
        return jnp.concatenate(terms, axis=0)

    def index(m, p):
        info = jnp.concatenate([chip_info(2 * p, m), chip_info(2 * p + 1, m)], axis=1)
        place, weight, eye = places(info, me * local_experts, local_experts)
        slot = grid((slots, 2 * chip), 0) - grid((slots, 2 * chip), 1) // micro * cap
        slot = slot.astype(F32)
        at = [slot == place[e] for e in range(local_experts)]
        picks[m, p] = jnp.concatenate([jnp.where(a, 1.0, 0.0) for a in at], axis=0).astype(BF16)
        mix = jnp.concatenate([jnp.where(at[e], weight[e], 0.0) for e in range(local_experts)], axis=0)
        cm[m, p] = lax.dot_general(eye, three_terms(mix), NT, preferred_element_type=F32).astype(BF16)

    def index_far(m, d):
        count = 2 * local_experts
        home = POS[SIGN[d] * (FAR - 1)]
        first = lax.rem(me - core + group - 2 * SIGN[d], group) * local_experts
        place, weight, eye = places(chip_info(home, m), first, count)
        slot = grid((16, chip), 0).astype(F32)
        mix = jnp.concatenate([jnp.where(slot == place[e], weight[e], 0.0) for e in range(count)], axis=0)
        turned = lax.dot_general(eye, three_terms(mix), NT, preferred_element_type=F32).astype(BF16)
        wide, tight = 16 * count, cap * count
        row, col = grid((TERMS * wide, TERMS * tight), 0), grid((TERMS * wide, TERMS * tight), 1)
        i = col % tight
        fm[m, d] = dot(turned, one((row // wide == col // tight) & (row % wide == i // cap * 16 + i % cap))).astype(BF16)

    def gather(m, p):
        for n in range(0, dim, WIDE):
            rows = dot(picks[m, p], xg[m, p, :, n:n + WIDE]).astype(BF16)
            for e in range(local_experts):
                xe[e, pl.ds(pl.multiple_of(p * slots, 16), slots), n:n + WIDE] = rows[e * slots:(e + 1) * slots]

    def experts(m, service):
        @pl.loop(0, local_experts)
        def _(e):
            s = lax.rem(e, 2)
            nxt = lax.rem(e + 2, local_experts)

            def after(step, copies):
                def start():
                    for cp in copies:
                        cp.start()

                if m == 0:
                    start()
                else:
                    pl.when(e + 2 < local_experts)(start)
                for at, fn in service.items():
                    if at[1] == step:
                        who = functools.reduce(lambda x, c: x & (core == c), at[2:], e == at[0])
                        pl.when(who)(fn)

            for f in range(2):
                landed(wgu.at[s, f], gu_sem.at[s, f])
                for c in range(0, GU_TILE, MXU):
                    a = dot(xe[e], wgu[s, f, 0, :, c:c + MXU])
                    b = dot(xe[e], wgu[s, f, 1, :, c:c + MXU])
                    hid[:, f * GU_TILE + c:f * GU_TILE + c + MXU] = (a * jax.nn.sigmoid(a) * b).astype(BF16)
                after(f, gu_copies(nxt, f))
            dn_copy(e).wait()
            for c in range(0, dim, MXU):
                o = dot(hid[...], wdn[s, :, c:c + MXU]).astype(BF16)
                for p in range(4):
                    eo[p, pl.ds(pl.multiple_of(e * slots, 16), slots), c:c + MXU] = o[p * slots:(p + 1) * slots]
            after(2, (dn_copy(nxt),))

    def combine(m, pos):
        p, top = pos // 2, (pos % 2) * chip
        if not isinstance(pos, int):
            top = pl.multiple_of(top, chip)
        gates = cm[m, p, pl.ds(top, chip)]
        for n in range(0, dim, WIDE):
            o = eo[p, :, n:n + WIDE]
            acc = dot(gates, jnp.concatenate([o, o, o], axis=0))
            part[pos - 1, 0, :, n:n + WIDE] = acc[:micro]
            part[pos - 1, 1, :, n:n + WIDE] = acc[micro:]

    def far_rows(m):
        count = local_experts * cap
        shape = (2 * count, local_experts * slots)
        row, col = grid(shape, 0), grid(shape, 1)
        i = row % count
        owner = jnp.where(row < count, core, other)
        take_row = one(col == i // cap * slots + owner * cap + i % cap)
        for n in range(0, dim, WIDE):
            o = dot(take_row, eo[0, :, n:n + WIDE]).astype(BF16)
            rows_out[m, core, :, n:n + WIDE] = o[:count]
            rows_sib[:, n:n + WIDE] = o[count:]
        sb_copy(m, 0).start()

    def sb_copy(m, pos):
        if isinstance(pos, int) and pos == 0:
            return remote(rows_sib, rows_out.at[m, core], sb_s.at[pos], sb_r.at[m, pos], sibling)
        return remote(part.at[pos - 1, other], sib.at[m, pos - 1], sb_s.at[pos], sb_r.at[m, pos], sibling)

    def back_item(d, j):
        dist, cols = BACK[j]
        return POS[SIGN[d] * dist], (cols if d == 0 else 1 - cols)

    def rs_copy(m, d, j):
        pos, r = back_item(d, j)
        cols = pl.ds(r * half, half)
        if j == 0:
            return remote(rows_out.at[m, :, :, cols], rows_in.at[d], rs_s.at[pos], rs_r.at[d, j], nbr[d])
        return remote(part.at[pos - 1, core, :, cols], inb.at[d, j - 1], rs_s.at[pos], rs_r.at[d, j], nbr[d])

    seen = set()

    def need_sib(m, pos):
        if (m, pos) not in seen:
            seen.add((m, pos))
            if pos == 0:
                landed(rows_out.at[m, other], sb_r.at[m, pos])
            else:
                sb_copy(m, pos).wait_recv()

    def back(m, j):
        for d in range(2):
            pos, r = back_item(d, j)
            need_sib(m, pos)
            if j > 0:
                cols = pl.ds(r * half, half)
                acc = part[pos - 1, core, :, cols] + sib[m, pos - 1, :, cols]
                if j == 2:
                    rs_copy(m, d, j - 2).wait_recv()
                    gates = fm[m, d, pl.ds(pl.multiple_of(core * micro, micro), micro)]
                    sent = jnp.concatenate([rows_in[d, 0], rows_in[d, 1]] * TERMS, axis=0)
                    acc = acc + dot(gates, sent)
                elif j > 2:
                    rs_copy(m, d, j - 2).wait_recv()
                    acc = acc + inb[d, j - 2 - 1]
                part[pos - 1, core, :, cols] = acc
            rs_copy(m, d, j).start()

    def finish(m, r):
        pos = HERE
        need_sib(m, pos)
        cols = pl.ds(r * half, half)
        acc = part[pos - 1, core, :, cols] + sib[m, pos - 1, :, cols]
        for d in range(2):
            j = SENDS - 2 if (r == 1) == (d == 0) else SENDS - 1
            if (m, d, j) not in seen:
                seen.add((m, d, j))
                rs_copy(m, d, j).wait_recv()
            acc = acc + inb[d, j - 1]
        rows = pl.ds(m * micro, micro)
        outv[rows, cols] = acc.astype(BF16)
        pltpu.make_async_copy(outv.at[rows, cols], out_hbm.at[rows, cols], st_sem).start()

    def combine_send(m, pos):
        combine(m, pos)
        sb_copy(m, pos).start()

    def combine_loop(m, first, last):
        @pl.loop(first, last)
        def _(pos):
            combine_send(m, pos)

    def part_free(m, pos):
        if pos == 0:
            landed(rows_sib, sb_s.at[pos])
            landed(rows_out.at[m], rs_s.at[pos])
            return
        landed(part.at[pos - 1, other], sb_s.at[pos])
        if pos != HERE:
            landed(part.at[pos - 1, core], rs_s.at[pos])

    def pair_wait(m, p):
        landed(xg.at[m, p, pl.ds(0, chip)], dx_r.at[m, p])

    def info_wait(p):
        landed(meta.at[pl.ds(2 * p, 2), 0], dm_r.at[p])

    loads = [pltpu.make_async_copy(x_hbm.at[pl.ds(m * micro, micro)], x_rows(m, HERE, core, 0, micro), ld_sem.at[m])
             for m in range(2)]
    loads.append(pltpu.make_async_copy(ids_hbm, ids_v, ld_sem.at[2]))
    loads.append(pltpu.make_async_copy(rw_hbm, rw_v, ld_sem.at[3]))
    for cp in loads:
        cp.start()

    def enter():
        barrier = pltpu.get_barrier_semaphore()
        for dev in (nbr[0], nbr[1], sibling):
            pl.semaphore_signal(barrier, inc=1, device_id={'ep': dev}, device_id_type=MESH)
        pl.semaphore_wait(barrier, 3)

    enter()
    loads[0].wait()

    send_own(0, 0, 1)
    for cp in loads[2:]:
        cp.wait()
    loads[1].wait()
    make_meta()
    for d in range(2):
        mt_copy(d, 0).start()
    dm_copy(HERE, core).start()
    send_own(0, 1, PIECES)
    load_weights()

    def prepare(p):
        info_wait(p)
        index(0, p)

    def fetch(m, p):
        pair_wait(m, p)
        gather(m, p)

    near, mid, wide, far = 3, 2, 1, 0
    mt_event(0)
    take(0, 0, PIECES)
    n = PIECES
    mt_event(1)
    take(0, n, n + 1)
    prepare(near)
    take(0, n + 1, n + 2)
    index(1, near)
    take(0, n + 2, n + 3)
    prepare(mid)
    take(0, n + 3, n + PIECES)
    pair_wait(0, near)
    n += PIECES
    mt_event(2)
    take(0, n, n + 1)
    gather(0, near)
    take(0, n + 1, n + 2)
    send_own(1, 0, PIECES)
    index(1, mid)
    take(0, n + 2, n + 3)
    prepare(wide)
    index_far(0, 0)
    take(0, n + 3, n + PIECES)
    fetch(0, mid)
    n += PIECES
    mt_event(last)
    index_far(0, 1)
    take(0, n, n + 1)
    prepare(far)
    take(0, n + 1, n + 2)
    pl.when(core == 1)(functools.partial(take, 1, 0, 1))
    fetch(0, wide)
    fetch(0, far)
    pl.when(core == 1)(functools.partial(take, 1, 1, 2))

    due = {}
    for c, first, steps in ((0, 0, (0, 1, 3, 4, 6, 7, 9, 10, 11)), (1, 2, (0, 2, 3, 4, 6, 7, 8, 10))):
        for n, step in enumerate(steps, first):
            due[divmod(step, STEPS) + (c,)] = functools.partial(take, 1, n, n + 1)
    experts(0, due)
    far_rows(0)
    n = (last - 1) * PIECES + 1
    pl.when(core == 0)(functools.partial(take, 1, n, n + 1))
    combine_loop(0, 2, FAR)
    back(0, 0)
    take(1, n + 1, last * PIECES)
    back(0, 1)
    combine_loop(0, FAR, FAR + 2)
    take(1, last * PIECES, last * PIECES + 2)
    combine_loop(0, FAR + 2, CHIPS)
    combine_send(0, HERE)
    for p in (wide, far):
        index(1, p)
    for p in range(PAIRS):
        fetch(1, p)

    for j in range(2, SENDS):
        for d in range(2):
            need_sib(0, back_item(d, j)[0])

    experts(1, {
        (0, 1): functools.partial(back, 0, 2),
        (2, 0): functools.partial(back, 0, 3),
    })
    part_free(0, 0)
    far_rows(1)
    back(0, 4)
    for d in range(2):
        index_far(1, d)
    part_free(0, 2)
    part_free(0, 3)
    combine_loop(1, 2, FAR)
    back(0, 5)
    back(0, 6)
    back(1, 0)
    back(1, 1)
    finish(0, 0)
    finish(0, 1)
    for pos in (HERE, *range(FAR, CHIPS)):
        part_free(0, pos)
    combine_loop(1, FAR, CHIPS)
    combine_send(1, HERE)
    for j in range(2, SENDS):
        back(1, j)
    finish(1, 0)
    finish(1, 1)

    def drain():
        for m in range(2):
            for d in range(2):
                landed(xg.at[m, 0, pl.ds(0, (3 * PIECES + PIECES // 2) * piece_rows)], ag_s.at[m, d])
            landed(xg.at[m, pl.ds(0, 2)], dx_s.at[m])
        landed(meta.at[pl.ds(0, 7), 0], mt_s)
        landed(meta.at[pl.ds(0, 8), 0], dm_s)
        for pos in range(CHIPS):
            part_free(1, pos)
        landed(outv, st_sem)

    drain()


def solution(mesh):
    group = mesh.shape['ep']

    def device_fn(act_in, router_w, expert_ids, w_gate, w_up, w_down):
        tokens, dim = act_in.shape
        local_experts, _, ffn = w_gate.shape
        micro = tokens // 2
        mean_load = micro * expert_ids.shape[1] // (local_experts * group)
        cap = mean_load + mean_load // 2
        slots = 4 * cap
        rows = local_experts * cap
        dma = pltpu.SemaphoreType.DMA
        scratch = [
            pltpu.VMEM((2, 4, 4 * micro, dim), BF16),
            pltpu.VMEM((8, 2, 2, 16, 2 * micro), F32),
            pltpu.VMEM(expert_ids.shape[::-1], jnp.int32),
            pltpu.VMEM(router_w.shape[::-1], BF16),
            pltpu.VMEM((tokens, 128), F32),
            pltpu.VMEM((local_experts, 4 * slots, dim), BF16),
            pltpu.VMEM((4 * slots, ffn), BF16),
            pltpu.VMEM((4, local_experts * slots, dim), BF16),
            pltpu.VMEM((2, 4, local_experts * slots, 4 * micro), BF16),
            pltpu.VMEM((2, 4, 4 * micro, 3 * local_experts * slots), BF16),
            pltpu.VMEM((2, 2, 2 * micro, 2 * TERMS * rows), BF16),
            pltpu.VMEM((2, 2, rows, dim), BF16),
            pltpu.VMEM((rows, dim), BF16),
            pltpu.VMEM((2, 2, rows, dim // 2), BF16),
            pltpu.VMEM((CHIPS - 1, 2, micro, dim), F32),
            pltpu.VMEM((2, CHIPS - 1, micro, dim), F32),
            pltpu.VMEM((2, SENDS - 1, micro, dim // 2), F32),
            pltpu.VMEM((tokens, dim), BF16),
            pltpu.VMEM((2, 2, 2, dim, GU_TILE), BF16),
            pltpu.VMEM((2, ffn, dim), BF16),
            dma((2, 2)), dma((2, 4, PIECES)),
            dma((2,)), dma((2, 4)),
            dma, dma((2, 4)),
            dma, dma((4,)),
            dma((8,)), dma((2, 7)),
            dma((8,)), dma((2, 8)),
            dma((2, 2)), dma((2,)), dma((4,)), dma,
        ]
        return pl.pallas_call(
            functools.partial(layer_kernel, group),
            out_shape=jax.ShapeDtypeStruct((tokens, dim), BF16),
            in_specs=[pl.BlockSpec(memory_space=pl.ANY)] * 6,
            out_specs=pl.BlockSpec(memory_space=pl.ANY),
            scratch_shapes=scratch,
            compiler_params=pltpu.CompilerParams(collective_id=0, has_side_effects=True,
                                                 vmem_limit_bytes=67043328),
            name='moe_layer',
        )(expert_ids.T, router_w.T, act_in, w_gate, w_up, w_down)

    row_spec = P(('dp', 'ep'), None)
    expert_spec = P('ep', None, None)
    return jax.shard_map(device_fn, mesh=mesh,
                         in_specs=(row_spec, P(None, None), row_spec, expert_spec, expert_spec, expert_spec),
                         out_specs=row_spec, check_vma=False)
```

```python
import functools

import jax
import jax.numpy as jnp
from jax import lax
from jax.experimental import pallas as pl
from jax.experimental.pallas import tpu as pltpu
from jax.sharding import PartitionSpec as P

MESH = pl.DeviceIdType.MESH
F32 = jnp.float32
BF16 = jnp.bfloat16

FAR = 4
ORDER = (FAR, 0, -3, 3, -2, 2, -1, 1)
POS = {away: i for i, away in enumerate(ORDER)}
POS[-FAR] = POS[FAR]
HERE = POS[0]
CHIPS = len(ORDER)
PAIRS = CHIPS // 2
SIGN = (1, -1)
TERMS = 3
NT = (((1,), (1,)), ((), ()))
BACK = ((FAR, 0),) + tuple((away, r) for away in range(FAR - 1, 0, -1) for r in (1, 0))
SENDS = len(BACK)
STEPS = 3
GU_TILE = 512
WIDE = 512
MXU = 256
PIECES = 4


def dot(a, b):
    return jnp.dot(a, b, preferred_element_type=F32)


def layer_kernel(group, ids_hbm, rw_hbm, x_hbm, wg_hbm, wu_hbm, wd_hbm, outv,
                 xg, meta, ids_v, rw_v, tp, xe, hid, eo, picks, cm, fm, rows_out, rows_sib, rows_in, part, sib, inb, wgu, wdn,
                 ag_s, ag_r, dx_s, dx_r, mt_s, mt_r, dm_s, dm_r, rs_s, sb_s, sb_r,
                 gu_sem, dn_sem, ld_sem):
    micro = outv.shape[0] // 2
    chip = 2 * micro
    dim = outv.shape[1]
    half = dim // 2
    last = FAR - 1
    piece_rows = micro // PIECES
    me = lax.axis_index('ep')
    core = lax.rem(me, 2)
    other = 1 - core
    nbr = (lax.rem(me + 2, group), lax.rem(me + group - 2, group))
    sibling = me + 1 - 2 * core
    local_experts = wg_hbm.shape[0]
    slots = xe.shape[1] // PAIRS
    cap = slots // (2 * 2)

    def remote(src, dst, ssem, rsem, dev):
        return pltpu.make_async_remote_copy(src_ref=src, dst_ref=dst, send_sem=ssem, recv_sem=rsem,
                                            device_id={'ep': dev}, device_id_type=MESH)

    def gu_copies(e, f):
        cols = pl.ds(f * GU_TILE, GU_TILE)
        s = lax.rem(e, 2)
        return (pltpu.make_async_copy(wg_hbm.at[e, :, cols], wgu.at[s, f, 0], gu_sem.at[s, f]),
                pltpu.make_async_copy(wu_hbm.at[e, :, cols], wgu.at[s, f, 1], gu_sem.at[s, f]))

    def dn_copy(e):
        return pltpu.make_async_copy(wd_hbm.at[e], wdn.at[lax.rem(e, 2)], dn_sem.at[lax.rem(e, 2)])

    def load_weights():
        for e in range(2):
            for f in range(2):
                for cp in gu_copies(e, f):
                    cp.start()
            dn_copy(e).start()

    def x_rows(m, pos, c, start, size):
        row = pl.multiple_of((pos % 2) * chip + c * micro + start, 16)
        return xg.at[m, pos // 2, pl.ds(row, size)]

    def ag_copy(m, d, k, i):
        start = ((i + d * PIECES // 2) % PIECES) * piece_rows
        src = x_rows(m, POS[-SIGN[d] * k], core, start, piece_rows)
        dst = x_rows(m, POS[-SIGN[d] * (k + 1)], core, start, piece_rows)
        return remote(src, dst, ag_s.at[m, d], ag_r.at[d, k, i], nbr[d])

    def ag_has(k, i):
        return k < last or i < PIECES // 2

    def landed(ref, sem):
        pltpu.make_async_copy(ref, ref, sem).wait()

    def dx_copy(m, pos, c):
        ref = x_rows(m, pos, c, 0, micro)
        return remote(ref, ref, dx_s.at[m], dx_r.at[m, pos // 2], sibling)

    def mt_copy(d, k):
        return remote(meta.at[POS[-SIGN[d] * k], core], meta.at[POS[-SIGN[d] * (k + 1)], core],
                      mt_s, mt_r.at[d, k], nbr[d])

    def mt_has(d, k):
        return k < last or d == 0

    def dm_copy(pos, c):
        return remote(meta.at[pos, c], meta.at[pos, c], dm_s, dm_r.at[pos // 2], sibling)

    def send_own(m, first, last):
        for i in range(first, last):
            for d in range(2):
                ag_copy(m, d, 0, i).start()
        if last == PIECES:
            dx_copy(m, HERE, core).start()

    def ag_event(m, k, i):
        for d in range(2):
            ag_copy(m, d, k, i).wait_recv()
            if k < last and ag_has(k + 1, i):
                ag_copy(m, d, k + 1, i).start()
        if k == last:
            for d in range(2):
                ref = x_rows(m, POS[FAR], core, (i + d * PIECES // 2) * piece_rows, piece_rows)
                remote(ref, ref, dx_s.at[m], dx_r.at[m, POS[FAR] // 2], sibling).start()
        elif i + 1 == PIECES:
            for d in range(2):
                dx_copy(m, POS[-SIGN[d] * (k + 1)], core).start()

    def take(m, first, after):
        for n in range(first, after):
            ag_event(m, n // PIECES, n % PIECES)

    def mt_event(k):
        for d in range(2):
            if mt_has(d, k):
                mt_copy(d, k).wait_recv()
                if k < last and mt_has(d, k + 1):
                    mt_copy(d, k + 1).start()
                dm_copy(POS[-SIGN[d] * (k + 1)], core).start()

    def make_meta():
        for m in range(2):
            rows = x_rows(m, HERE, core, 0, micro)
            tp[m * micro:(m + 1) * micro, 0:rw_v.shape[0]] = lax.dot_general(
                rows[...], rw_v[...], NT, preferred_element_type=F32)
        ids = ids_v[...].astype(F32)
        expert = lax.broadcasted_iota(jnp.int32, (rw_v.shape[0], chip), 0).astype(F32)
        logits = tp[...].T[0:rw_v.shape[0]]
        picked = []
        for j in range(8):
            picked.append(jnp.sum(jnp.where(expert == ids[j:j + 1], logits, 0.0), axis=0, keepdims=True))
        picked = jnp.concatenate(picked, axis=0)
        top = jnp.exp(picked - jnp.max(picked, axis=0, keepdims=True))
        gates = top / jnp.sum(top, axis=0, keepdims=True)
        both = jnp.concatenate([ids, gates], axis=0)
        turned = pltpu.roll(both, micro, 1)
        mine = lax.broadcasted_iota(jnp.int32, both.shape, 1) // micro == core
        for m in range(2):
            meta[HERE, core, m] = jnp.where(mine, jnp.where(core == m, both, turned), 0.0)

    def grid(shape, axis):
        return lax.broadcasted_iota(jnp.int32, shape, axis)

    def one(mask):
        return jnp.where(mask, 1.0, 0.0).astype(BF16)

    def chip_info(pos, m):
        return meta[pos, 0, m] + meta[pos, 1, m]

    def places(info, first, count):
        token = info.shape[1]
        ids, gates = info[0:8], info[8:16]
        chosen, weight = [], []
        for e in range(count):
            hit = ids == (first + e).astype(F32)
            chosen.append(jnp.sum(jnp.where(hit, 1.0, 0.0), axis=0, keepdims=True))
            weight.append(jnp.sum(jnp.where(hit, gates, 0.0), axis=0, keepdims=True))
        stacked = jnp.concatenate(chosen + [jnp.zeros((info.shape[0] - count, token), F32)], axis=0)
        row, col = grid((token, token), 0), grid((token, token), 1)
        rank = dot(stacked.astype(BF16), one((row < col) & (row // micro == col // micro)))
        return [jnp.where(chosen[e] > 0.5, rank[e:e + 1], -slots) for e in range(count)], weight, one(row == col)

    def three_terms(rest):
        terms = []
        for i in range(TERMS):
            terms.append(rest.astype(BF16))
            rest = rest - terms[i].astype(F32)
        return jnp.concatenate(terms, axis=0)

    def index(m, p):
        info = jnp.concatenate([chip_info(2 * p, m), chip_info(2 * p + 1, m)], axis=1)
        place, weight, eye = places(info, me * local_experts, local_experts)
        slot = grid((slots, 2 * chip), 0) - grid((slots, 2 * chip), 1) // micro * cap
        slot = slot.astype(F32)
        at = [slot == place[e] for e in range(local_experts)]
        picks[m, p] = jnp.concatenate([jnp.where(a, 1.0, 0.0) for a in at], axis=0).astype(BF16)
        mix = jnp.concatenate([jnp.where(at[e], weight[e], 0.0) for e in range(local_experts)], axis=0)
        cm[m, p] = lax.dot_general(eye, three_terms(mix), NT, preferred_element_type=F32).astype(BF16)

    def index_far(m, d):
        count = 2 * local_experts
        home = POS[SIGN[d] * (FAR - 1)]
        first = lax.rem(me - core + group - 2 * SIGN[d], group) * local_experts
        place, weight, eye = places(chip_info(home, m), first, count)
        slot = grid((16, chip), 0).astype(F32)
        mix = jnp.concatenate([jnp.where(slot == place[e], weight[e], 0.0) for e in range(count)], axis=0)
        turned = lax.dot_general(eye, three_terms(mix), NT, preferred_element_type=F32).astype(BF16)
        wide, tight = 16 * count, cap * count
        row, col = grid((TERMS * wide, TERMS * tight), 0), grid((TERMS * wide, TERMS * tight), 1)
        i = col % tight
        fm[m, d] = dot(turned, one((row // wide == col // tight) & (row % wide == i // cap * 16 + i % cap))).astype(BF16)

    def gather(m, p):
        for n in range(0, dim, WIDE):
            rows = dot(picks[m, p], xg[m, p, :, n:n + WIDE]).astype(BF16)
            for e in range(local_experts):
                xe[e, pl.ds(pl.multiple_of(p * slots, 16), slots), n:n + WIDE] = rows[e * slots:(e + 1) * slots]

    def experts(m, service):
        @pl.loop(0, local_experts)
        def _(e):
            s = lax.rem(e, 2)
            nxt = lax.rem(e + 2, local_experts)

            def after(step, copies):
                def start():
                    for cp in copies:
                        cp.start()

                if m == 0:
                    start()
                else:
                    pl.when(e + 2 < local_experts)(start)
                for at, fn in service.items():
                    if at[1] == step:
                        who = functools.reduce(lambda x, c: x & (core == c), at[2:], e == at[0])
                        pl.when(who)(fn)

            for f in range(2):
                landed(wgu.at[s, f], gu_sem.at[s, f])
                for c in range(0, GU_TILE, MXU):
                    a = dot(xe[e], wgu[s, f, 0, :, c:c + MXU])
                    b = dot(xe[e], wgu[s, f, 1, :, c:c + MXU])
                    hid[:, f * GU_TILE + c:f * GU_TILE + c + MXU] = (a * jax.nn.sigmoid(a) * b).astype(BF16)
                after(f, gu_copies(nxt, f))
            dn_copy(e).wait()
            for c in range(0, dim, MXU):
                o = dot(hid[...], wdn[s, :, c:c + MXU]).astype(BF16)
                for p in range(4):
                    eo[p, pl.ds(pl.multiple_of(e * slots, 16), slots), c:c + MXU] = o[p * slots:(p + 1) * slots]
            after(2, (dn_copy(nxt),))

    def combine(m, pos):
        p, top = pos // 2, (pos % 2) * chip
        if not isinstance(pos, int):
            top = pl.multiple_of(top, chip)
        gates = cm[m, p, pl.ds(top, chip)]
        for n in range(0, dim, WIDE):
            o = eo[p, :, n:n + WIDE]
            acc = dot(gates, jnp.concatenate([o, o, o], axis=0))
            part[pos - 1, 0, :, n:n + WIDE] = acc[:micro]
            part[pos - 1, 1, :, n:n + WIDE] = acc[micro:]

    def far_rows(m):
        count = local_experts * cap
        shape = (2 * count, local_experts * slots)
        row, col = grid(shape, 0), grid(shape, 1)
        i = row % count
        owner = jnp.where(row < count, core, other)
        take_row = one(col == i // cap * slots + owner * cap + i % cap)
        for n in range(0, dim, WIDE):
            o = dot(take_row, eo[0, :, n:n + WIDE]).astype(BF16)
            rows_out[m, core, :, n:n + WIDE] = o[:count]
            rows_sib[:, n:n + WIDE] = o[count:]
        sb_copy(m, 0).start()

    def key(pos):
        return pos if isinstance(pos, int) and pos < 2 else pos // 2 + 1

    def sb_copy(m, pos):
        if isinstance(pos, int) and pos == 0:
            return remote(rows_sib, rows_out.at[m, core], sb_s.at[key(pos)], sb_r.at[m, key(pos)], sibling)
        return remote(part.at[pos - 1, other], sib.at[m, pos - 1], sb_s.at[key(pos)], sb_r.at[m, key(pos)], sibling)

    def back_item(d, j):
        dist, cols = BACK[j]
        return POS[SIGN[d] * dist], (cols if d == 0 else 1 - cols)

    def rs_copy(m, d, j):
        pos, r = back_item(d, j)
        cols = pl.ds(r * half, half)
        if j == 0:
            return remote(rows_out.at[m, :, :, cols], rows_in.at[d], rs_s.at[key(pos)], ag_r.at[d, j // PIECES, j % PIECES], nbr[d])
        return remote(part.at[pos - 1, core, :, cols], inb.at[d, j - 1], rs_s.at[key(pos)], ag_r.at[d, j // PIECES, j % PIECES], nbr[d])

    seen = set()

    def need_sib(m, pos):
        if (m, key(pos)) not in seen:
            seen.add((m, key(pos)))
            if pos == 0:
                came = rows_out.at[m, other]
            elif pos == HERE:
                came = sib.at[m, 0]
            else:
                came = sib.at[m, pl.ds(pos - pos % 2 - 1, 2)]
            landed(came, sb_r.at[m, key(pos)])

    def back(m, j):
        for d in range(2):
            pos, r = back_item(d, j)
            need_sib(m, pos)
            if j > 0:
                cols = pl.ds(r * half, half)
                acc = part[pos - 1, core, :, cols] + sib[m, pos - 1, :, cols]
                if j == 2:
                    rs_copy(m, d, j - 2).wait_recv()
                    gates = fm[m, d, pl.ds(pl.multiple_of(core * micro, micro), micro)]
                    sent = jnp.concatenate([rows_in[d, 0], rows_in[d, 1]] * TERMS, axis=0)
                    acc = acc + dot(gates, sent)
                elif j > 2:
                    rs_copy(m, d, j - 2).wait_recv()
                    acc = acc + inb[d, j - 2 - 1]
                part[pos - 1, core, :, cols] = acc
            rs_copy(m, d, j).start()

    def finish(m, r):
        pos = HERE
        need_sib(m, pos)
        cols = pl.ds(r * half, half)
        acc = part[pos - 1, core, :, cols] + sib[m, pos - 1, :, cols]
        for d in range(2):
            j = SENDS - 2 if (r == 1) == (d == 0) else SENDS - 1
            if (m, d, j) not in seen:
                seen.add((m, d, j))
                rs_copy(m, d, j).wait_recv()
            acc = acc + inb[d, j - 1]
        rows = pl.ds(m * micro, micro)
        outv[rows, cols] = acc.astype(BF16)

    def combine_send(m, pos):
        combine(m, pos)
        sb_copy(m, pos).start()

    def combine_loop(m, first, last):
        @pl.loop(first, last)
        def _(pos):
            combine_send(m, pos)

    def part_free(m, pos):
        if pos == 0:
            landed(rows_sib, sb_s.at[pos])
            landed(rows_out.at[m], rs_s.at[pos])
        elif pos == HERE:
            landed(part.at[0, other], sb_s.at[pos])
        else:
            landed(part.at[pl.ds(pos - 1, 2), other], sb_s.at[key(pos)])
            landed(part.at[pl.ds(pos - 1, 2), core], rs_s.at[key(pos)])

    def pair_wait(m, p):
        landed(xg.at[m, p, pl.ds(0, chip)], dx_r.at[m, p])

    def info_wait(p):
        landed(meta.at[pl.ds(2 * p, 2), 0], dm_r.at[p])

    loads = [pltpu.make_async_copy(x_hbm.at[pl.ds(m * micro, micro)], x_rows(m, HERE, core, 0, micro), ld_sem.at[m])
             for m in range(2)]
    loads.append(pltpu.make_async_copy(ids_hbm, ids_v, ld_sem.at[2]))
    loads.append(pltpu.make_async_copy(rw_hbm, rw_v, ld_sem.at[3]))
    for cp in loads:
        cp.start()

    def enter():
        barrier = pltpu.get_barrier_semaphore()
        for dev in (nbr[0], nbr[1], sibling):
            pl.semaphore_signal(barrier, inc=1, device_id={'ep': dev}, device_id_type=MESH)
        pl.semaphore_wait(barrier, 3)

    enter()
    loads[0].wait()

    send_own(0, 0, 1)
    for cp in loads[2:]:
        cp.wait()
    loads[1].wait()
    make_meta()
    for d in range(2):
        mt_copy(d, 0).start()
    dm_copy(HERE, core).start()
    send_own(0, 1, PIECES)
    load_weights()

    def prepare(p):
        info_wait(p)
        index(0, p)

    def fetch(m, p):
        pair_wait(m, p)
        gather(m, p)

    near, mid, wide, far = 3, 2, 1, 0
    mt_event(0)
    take(0, 0, PIECES)
    n = PIECES
    mt_event(1)
    take(0, n, n + 1)
    prepare(near)
    take(0, n + 1, n + 2)
    index(1, near)
    take(0, n + 2, n + 3)
    prepare(mid)
    take(0, n + 3, n + PIECES)
    pair_wait(0, near)
    n += PIECES
    mt_event(2)
    take(0, n, n + 1)
    gather(0, near)
    take(0, n + 1, n + 2)
    send_own(1, 0, PIECES)
    index(1, mid)
    take(0, n + 2, n + 3)
    prepare(wide)
    index_far(0, 0)
    take(0, n + 3, n + PIECES)
    fetch(0, mid)
    n += PIECES
    mt_event(last)
    index_far(0, 1)
    take(0, n, n + 1)
    prepare(far)
    take(0, n + 1, n + 2)
    pl.when(core == 1)(functools.partial(take, 1, 0, 1))
    fetch(0, wide)
    fetch(0, far)
    pl.when(core == 1)(functools.partial(take, 1, 1, 2))

    due = {}
    for c, first, steps in ((0, 0, (0, 1, 3, 4, 6, 7, 9, 10, 11)), (1, 2, (0, 2, 3, 4, 6, 7, 8, 10))):
        for n, step in enumerate(steps, first):
            due[divmod(step, STEPS) + (c,)] = functools.partial(take, 1, n, n + 1)
    experts(0, due)
    far_rows(0)
    n = (last - 1) * PIECES + 1
    pl.when(core == 0)(functools.partial(take, 1, n, n + 1))
    combine_loop(0, 2, FAR)
    back(0, 0)
    take(1, n + 1, last * PIECES)
    back(0, 1)
    combine_loop(0, FAR, FAR + 2)
    take(1, last * PIECES, last * PIECES + 2)
    combine_loop(0, FAR + 2, CHIPS)
    combine_send(0, HERE)
    for p in (wide, far):
        index(1, p)
    for p in range(PAIRS):
        fetch(1, p)

    for j in range(2, SENDS):
        for d in range(2):
            need_sib(0, back_item(d, j)[0])

    experts(1, {
        (0, 1): functools.partial(back, 0, 2),
        (2, 0): functools.partial(back, 0, 3),
    })
    part_free(0, 0)
    far_rows(1)
    back(0, 4)
    for d in range(2):
        index_far(1, d)
    part_free(0, 2)
    combine_loop(1, 2, FAR)
    back(0, 5)
    back(0, 6)
    back(1, 0)
    back(1, 1)
    finish(0, 0)
    finish(0, 1)
    for pos in (HERE, *range(FAR, CHIPS, 2)):
        part_free(0, pos)
    combine_loop(1, FAR, CHIPS)
    combine_send(1, HERE)
    for j in range(2, SENDS):
        back(1, j)
    finish(1, 0)
    finish(1, 1)

    def drain():
        for m in range(2):
            for d in range(2):
                landed(xg.at[m, 0, pl.ds(0, (3 * PIECES + PIECES // 2) * piece_rows)], ag_s.at[m, d])
            landed(xg.at[m, pl.ds(0, 2)], dx_s.at[m])
        landed(meta.at[pl.ds(0, 7), 0], mt_s)
        landed(meta.at[pl.ds(0, 8), 0], dm_s)
        for pos in (0, HERE, *range(2, CHIPS, 2)):
            part_free(1, pos)

    drain()


def solution(mesh):
    group = mesh.shape['ep']

    def device_fn(act_in, router_w, expert_ids, w_gate, w_up, w_down):
        tokens, dim = act_in.shape
        local_experts, _, ffn = w_gate.shape
        micro = tokens // 2
        mean_load = micro * expert_ids.shape[1] // (local_experts * group)
        cap = mean_load + mean_load // 2
        slots = 4 * cap
        rows = local_experts * cap
        dma = pltpu.SemaphoreType.DMA
        scratch = [
            pltpu.VMEM((2, 4, 4 * micro, dim), BF16),
            pltpu.VMEM((8, 2, 2, 16, 2 * micro), F32),
            pltpu.VMEM(expert_ids.shape[::-1], jnp.int32),
            pltpu.VMEM(router_w.shape[::-1], BF16),
            pltpu.VMEM((tokens, 128), F32),
            pltpu.VMEM((local_experts, 4 * slots, dim), BF16),
            pltpu.VMEM((4 * slots, ffn), BF16),
            pltpu.VMEM((4, local_experts * slots, dim), BF16),
            pltpu.VMEM((2, 4, local_experts * slots, 4 * micro), BF16),
            pltpu.VMEM((2, 4, 4 * micro, 3 * local_experts * slots), BF16),
            pltpu.VMEM((2, 2, 2 * micro, 2 * TERMS * rows), BF16),
            pltpu.VMEM((2, 2, rows, dim), BF16),
            pltpu.VMEM((rows, dim), BF16),
            pltpu.VMEM((2, 2, rows, dim // 2), BF16),
            pltpu.VMEM((CHIPS - 1, 2, micro, dim), F32),
            pltpu.VMEM((2, CHIPS - 1, micro, dim), F32),
            pltpu.VMEM((2, SENDS - 1, micro, dim // 2), F32),
            pltpu.VMEM((2, 2, 2, dim, GU_TILE), BF16),
            pltpu.VMEM((2, ffn, dim), BF16),
            dma((2, 2)), dma((2, 4, PIECES)),
            dma((2,)), dma((2, 4)),
            dma, dma((2, 4)),
            dma, dma((4,)),
            dma((5,)),
            dma((5,)), dma((2, 5)),
            dma((2, 2)), dma((2,)), dma((4,)),
        ]
        return pl.pallas_call(
            functools.partial(layer_kernel, group),
            out_shape=pltpu.VMEM((tokens, dim), BF16),
            in_specs=[pl.BlockSpec(memory_space=pl.ANY)] * 6,
            out_specs=pl.BlockSpec(memory_space=pltpu.VMEM),
            scratch_shapes=scratch,
            compiler_params=pltpu.CompilerParams(collective_id=0, has_side_effects=True,
                                                 vmem_limit_bytes=66060288),
            name='moe_layer',
        )(expert_ids.T, router_w.T, act_in, w_gate, w_up, w_down)

    row_spec = P(('dp', 'ep'), None)
    expert_spec = P('ep', None, None)
    return jax.shard_map(device_fn, mesh=mesh,
                         in_specs=(row_spec, P(None, None), row_spec, expert_spec, expert_spec, expert_spec),
                         out_specs=row_spec, check_vma=False)
```

```python
import functools

import jax
import jax.numpy as jnp
from jax import lax
from jax.experimental import pallas as pl
from jax.experimental.pallas import tpu as pltpu
from jax.sharding import PartitionSpec as P

MESH = pl.DeviceIdType.MESH
F32 = jnp.float32
BF16 = jnp.bfloat16

FAR = 4
ORDER = (FAR, 0, -3, 3, -2, 2, -1, 1)
POS = {away: i for i, away in enumerate(ORDER)}
POS[-FAR] = POS[FAR]
HERE = POS[0]
CHIPS = len(ORDER)
PAIRS = CHIPS // 2
SIGN = (1, -1)
TERMS = 3
NT = (((1,), (1,)), ((), ()))
BACK = ((FAR, 0),) + tuple((away, r) for away in range(FAR - 1, 0, -1) for r in (1, 0))
SENDS = len(BACK)
STEPS = 3
GU_TILE = 512
WIDE = 512
MXU = 256
PIECES = 4


def dot(a, b):
    return jnp.dot(a, b, preferred_element_type=F32)


def layer_kernel(group, ids_hbm, rw_hbm, x_hbm, wg_hbm, wu_hbm, wd_hbm, outv,
                 xg, meta, ids_v, xe, hid, eo, picks, cm, fm, rows_out, rows_sib, rows_in, near_out, near_sib, near_in, part, sib, inb, wgu, wdn,
                 ag_s, ag_r, dx_s, dx_r, mt_s, mt_r, dm_s, dm_r, rs_s, sb_s, sb_r, nr_s, nb_s, nb_r,
                 gu_sem, dn_sem, ld_sem):
    micro = outv.shape[0] // 2
    chip = 2 * micro
    dim = outv.shape[1]
    half = dim // 2
    last = FAR - 1
    piece_rows = micro // PIECES
    me = lax.axis_index('ep')
    core = lax.rem(me, 2)
    other = 1 - core
    nbr = (lax.rem(me + 2, group), lax.rem(me + group - 2, group))
    sibling = me + 1 - 2 * core
    local_experts = wg_hbm.shape[0]
    slots = xe.shape[1] // PAIRS
    cap = slots // (2 * 2)

    def remote(src, dst, ssem, rsem, dev):
        return pltpu.make_async_remote_copy(src_ref=src, dst_ref=dst, send_sem=ssem, recv_sem=rsem,
                                            device_id={'ep': dev}, device_id_type=MESH)

    def gu_copies(e, f):
        cols = pl.ds(f * GU_TILE, GU_TILE)
        s = lax.rem(e, 2)
        return (pltpu.make_async_copy(wg_hbm.at[e, :, cols], wgu.at[s, f, 0], gu_sem.at[s, f]),
                pltpu.make_async_copy(wu_hbm.at[e, :, cols], wgu.at[s, f, 1], gu_sem.at[s, f]))

    def dn_copy(e):
        return pltpu.make_async_copy(wd_hbm.at[e], wdn.at[lax.rem(e, 2)], dn_sem.at[lax.rem(e, 2)])

    def load_weights():
        for e in range(2):
            for f in range(2):
                for cp in gu_copies(e, f):
                    cp.start()
            dn_copy(e).start()

    def x_rows(m, pos, c, start, size):
        row = pl.multiple_of((pos % 2) * chip + c * micro + start, 16)
        return xg.at[m, pos // 2, pl.ds(row, size)]

    def ag_copy(m, d, k, i):
        start = ((i + d * PIECES // 2) % PIECES) * piece_rows
        src = x_rows(m, POS[-SIGN[d] * k], core, start, piece_rows)
        dst = x_rows(m, POS[-SIGN[d] * (k + 1)], core, start, piece_rows)
        return remote(src, dst, ag_s.at[m, d], ag_r.at[d, k, i], nbr[d])

    def ag_has(k, i):
        return k < last or i < PIECES // 2

    def landed(ref, sem):
        pltpu.make_async_copy(ref, ref, sem).wait()

    def dx_copy(m, pos, c):
        ref = x_rows(m, pos, c, 0, micro)
        return remote(ref, ref, dx_s.at[m], dx_r.at[m, pos // 2], sibling)

    def mt_copy(d, k):
        return remote(meta.at[POS[-SIGN[d] * k], core], meta.at[POS[-SIGN[d] * (k + 1)], core],
                      mt_s, mt_r.at[d, k], nbr[d])

    def mt_has(d, k):
        return k < last or d == 0

    def dm_copy(pos, c):
        return remote(meta.at[pos, c], meta.at[pos, c], dm_s, dm_r.at[pos // 2], sibling)

    def send_own(m, first, last):
        for i in range(first, last):
            for d in range(2):
                ag_copy(m, d, 0, i).start()
        if last == PIECES:
            dx_copy(m, HERE, core).start()

    def ag_event(m, k, i):
        for d in range(2):
            ag_copy(m, d, k, i).wait_recv()
            if k < last and ag_has(k + 1, i):
                ag_copy(m, d, k + 1, i).start()
        if k == last:
            for d in range(2):
                ref = x_rows(m, POS[FAR], core, (i + d * PIECES // 2) * piece_rows, piece_rows)
                remote(ref, ref, dx_s.at[m], dx_r.at[m, POS[FAR] // 2], sibling).start()
        elif i + 1 == PIECES:
            for d in range(2):
                dx_copy(m, POS[-SIGN[d] * (k + 1)], core).start()

    def take(m, first, count=1):
        for n in range(first, first + count):
            ag_event(m, n // PIECES, n % PIECES)

    def mt_event(k):
        for d in range(2):
            if mt_has(d, k):
                mt_copy(d, k).wait_recv()
                if k < last and mt_has(d, k + 1):
                    mt_copy(d, k + 1).start()
                dm_copy(POS[-SIGN[d] * (k + 1)], core).start()

    rw_v = xe.at[local_experts - 1, pl.ds(0, rw_hbm.shape[0])]

    def make_meta():
        for m in range(2):
            rows = x_rows(m, HERE, core, 0, micro)
            part[0, m, :, 0:rw_v.shape[0]] = lax.dot_general(rows[...], rw_v[...], NT, preferred_element_type=F32)
        ids = ids_v[...].astype(F32)
        expert = lax.broadcasted_iota(jnp.int32, (rw_v.shape[0], chip), 0).astype(F32)
        logits = jnp.concatenate([part[0, m, :, 0:chip] for m in range(2)], axis=0).T[0:rw_v.shape[0]]
        picked = []
        for j in range(8):
            picked.append(jnp.sum(jnp.where(expert == ids[j:j + 1], logits, 0.0), axis=0, keepdims=True))
        picked = jnp.concatenate(picked, axis=0)
        top = jnp.exp(picked - jnp.max(picked, axis=0, keepdims=True))
        gates = top / jnp.sum(top, axis=0, keepdims=True)
        both = jnp.concatenate([ids, gates], axis=0)
        turned = pltpu.roll(both, micro, 1)
        mine = lax.broadcasted_iota(jnp.int32, both.shape, 1) // micro == core
        for m in range(2):
            meta[HERE, core, m] = jnp.where(mine, jnp.where(core == m, both, turned), 0.0)

    def grid(shape, axis):
        return lax.broadcasted_iota(jnp.int32, shape, axis)

    def one(mask):
        return jnp.where(mask, 1.0, 0.0).astype(BF16)

    def chip_info(pos, m):
        return meta[pos, 0, m] + meta[pos, 1, m]

    def places(info, first, count):
        token = info.shape[1]
        ids, gates = jnp.split(info, 2)
        chosen, weight = [], []
        for e in range(count):
            hit = ids == (first + e).astype(F32)
            chosen.append(jnp.sum(jnp.where(hit, 1.0, 0.0), axis=0, keepdims=True))
            weight.append(jnp.sum(jnp.where(hit, gates, 0.0), axis=0, keepdims=True))
        stacked = jnp.concatenate(chosen + [jnp.zeros((info.shape[0] - count, token), F32)], axis=0)
        row, col = grid((token, token), 0), grid((token, token), 1)
        rank = dot(stacked.astype(BF16), one((row < col) & (row // micro == col // micro)))
        return [jnp.where(chosen[e] > 0.5, rank[e:e + 1], -slots) for e in range(count)], weight, one(row == col)

    def three_terms(rest):
        terms = []
        for i in range(TERMS):
            terms.append(rest.astype(BF16))
            rest = rest - terms[i].astype(F32)
        return jnp.concatenate(terms, axis=0)

    def index(m, p):
        info = jnp.concatenate([chip_info(2 * p, m), chip_info(2 * p + 1, m)], axis=1)
        place, weight, eye = places(info, me * local_experts, local_experts)
        slot = grid((slots, 2 * chip), 0) - grid((slots, 2 * chip), 1) // micro * cap
        slot = slot.astype(F32)
        at = [slot == place[e] for e in range(local_experts)]
        picks[p] = jnp.concatenate([jnp.where(a, 1.0, 0.0) for a in at], axis=0).astype(BF16)
        mix = jnp.concatenate([jnp.where(at[e], weight[e], 0.0) for e in range(local_experts)], axis=0)
        cm[m, p] = lax.dot_general(eye, three_terms(mix), NT, preferred_element_type=F32).astype(BF16)

    def index_far(m, d, step):
        count = 2 * local_experts
        home = POS[SIGN[d] * (FAR - 1 - step)]
        first = lax.rem(me - core + group - 2 * SIGN[d], group) * local_experts
        place, weight, eye = places(chip_info(home, m), first, count)
        slot = grid((16, chip), 0).astype(F32)
        mix = jnp.concatenate([jnp.where(slot == place[e], weight[e], 0.0) for e in range(count)], axis=0)
        turned = lax.dot_general(eye, three_terms(mix), NT, preferred_element_type=F32).astype(BF16)
        wide, tight = 16 * count, cap * count
        row, col = grid((TERMS * wide, TERMS * tight), 0), grid((TERMS * wide, TERMS * tight), 1)
        i = col % tight
        fm[step, d] = dot(turned, one((row // wide == col // tight) & (row % wide == i // cap * 16 + i % cap))).astype(BF16)

    def gather(m, p):
        for n in range(0, dim, WIDE):
            rows = dot(picks[p], xg[m, p, :, n:n + WIDE]).astype(BF16)
            for e in range(local_experts):
                xe[e, pl.ds(pl.multiple_of(p * slots, 16), slots), n:n + WIDE] = rows[e * slots:(e + 1) * slots]

    def experts(m, service):
        @pl.loop(0, local_experts)
        def _(e):
            s = lax.rem(e, 2)
            nxt = lax.rem(e + 2, local_experts)

            def after(step, copies):
                def start():
                    for cp in copies:
                        cp.start()

                if m == 0:
                    start()
                else:
                    pl.when(e + 2 < local_experts)(start)
                for at, fn in service.items():
                    if at[1] == step:
                        who = functools.reduce(lambda x, c: x & (core == c), at[2:], e == at[0])
                        pl.when(who)(fn)

            for f in range(2):
                landed(wgu.at[s, f], gu_sem.at[s, f])
                for c in range(0, GU_TILE, MXU):
                    a = dot(xe[e], wgu[s, f, 0, :, c:c + MXU])
                    b = dot(xe[e], wgu[s, f, 1, :, c:c + MXU])
                    hid[:, f * GU_TILE + c:f * GU_TILE + c + MXU] = (a * jax.nn.sigmoid(a) * b).astype(BF16)
                after(f, gu_copies(nxt, f))
            dn_copy(e).wait()
            for c in range(0, dim, MXU):
                o = dot(hid[...], wdn[s, :, c:c + MXU]).astype(BF16)
                for p in range(4):
                    eo[p, pl.ds(pl.multiple_of(e * slots, 16), slots), c:c + MXU] = o[p * slots:(p + 1) * slots]
            after(2, (dn_copy(nxt),))

    def sum_cols(pos):
        if isinstance(pos, int) and pos // 2 == 1:
            first = back_item(1 - pos % 2, 2)[1] * half
            return first, first + half
        return 0, dim

    def combine(m, pos):
        p, top = pos // 2, (pos % 2) * chip
        if not isinstance(pos, int):
            top = pl.multiple_of(top, chip)
        gates = cm[m, p, pl.ds(top, chip)]
        first, after = sum_cols(pos)
        for n in range(first, after, WIDE):
            o = eo[p, :, n:n + WIDE]
            acc = dot(gates, jnp.concatenate([o, o, o], axis=0))
            part[pos - 1, 0, :, n:n + WIDE] = acc[:micro]
            part[pos - 1, 1, :, n:n + WIDE] = acc[micro:]

    def raw_rows(pos, first, after, own, sent):
        count = local_experts * cap
        shape = (2 * count, local_experts * slots)
        row, col = grid(shape, 0), grid(shape, 1)
        i = row % count
        owner = jnp.where(row < count, core, other) + pos % 2 * 2
        take_row = one(col == i // cap * slots + owner * cap + i % cap)
        for n in range(first, after, WIDE):
            o = dot(take_row, eo[pos // 2, :, n:n + WIDE]).astype(BF16)
            own[:, n - first:n - first + WIDE] = o[:count]
            sent[:, n - first:n - first + WIDE] = o[count:]

    def far_rows(m):
        raw_rows(0, 0, dim, rows_out.at[m, core], rows_sib)
        sb_copy(m, 0).start()

    def near_rows(m):
        for d in range(2):
            pos, r = back_item(d, 1)
            raw_rows(pos, r * half, r * half + half, near_out.at[m, d, core], near_sib.at[d])
            remote(near_sib.at[d], near_out.at[m, d, core], nb_s.at[d], nb_r.at[m, d], sibling).start()

    def key(pos):
        return pos if isinstance(pos, int) and pos < 2 else pos // 2 + 1

    def sb_copy(m, pos):
        if isinstance(pos, int) and pos == 0:
            return remote(rows_sib, rows_out.at[m, core], sb_s.at[key(pos)], sb_r.at[m, key(pos)], sibling)
        if isinstance(pos, int):
            first, after = sum_cols(pos)
            cols = pl.ds(first, after - first)
            return remote(part.at[pos - 1, other, :, cols], sib.at[m, pos - 1, :, cols],
                          sb_s.at[key(pos)], sb_r.at[m, key(pos)], sibling)
        return remote(part.at[pos - 1, other], sib.at[m, pos - 1], sb_s.at[key(pos)], sb_r.at[m, key(pos)], sibling)

    def back_item(d, j):
        dist, cols = BACK[j]
        return POS[SIGN[d] * dist], (cols if d == 0 else 1 - cols)

    def rs_copy(m, d, j):
        pos, r = back_item(d, j)
        cols = pl.ds(r * half, half)
        if j == 0:
            return remote(rows_out.at[m, :, :, cols], rows_in.at[d], rs_s.at[key(pos)], ag_r.at[d, j // PIECES, j % PIECES], nbr[d])
        if j == 1:
            return remote(near_out.at[m, d], near_in.at[d], nr_s, ag_r.at[d, j // PIECES, j % PIECES], nbr[d])
        return remote(part.at[pos - 1, core, :, cols], inb.at[d, j - 2], rs_s.at[key(pos)], ag_r.at[d, j // PIECES, j % PIECES], nbr[d])

    seen = set()

    def need_sib(m, pos):
        if (m, key(pos)) not in seen:
            seen.add((m, key(pos)))
            if pos == 0:
                came = rows_out.at[m, other]
            elif pos == HERE:
                came = sib.at[m, 0]
            elif pos // 2 == 1:
                came = sib.at[m, 1]
            else:
                came = sib.at[m, pl.ds(pos - pos % 2 - 1, 2)]
            landed(came, sb_r.at[m, key(pos)])

    def back(m, j):
        for d in range(2):
            pos, r = back_item(d, j)
            if j == 1:
                landed(near_out.at[m, d, other], nb_r.at[m, d])
            else:
                need_sib(m, pos)
            if j > 1:
                cols = pl.ds(r * half, half)
                acc = part[pos - 1, core, :, cols] + sib[m, pos - 1, :, cols]
                rs_copy(m, d, j - 2).wait_recv()
                if j < FAR:
                    gates = fm[j - 2, d, pl.ds(pl.multiple_of(core * micro, micro), micro)]
                    came = near_in if j == last else rows_in
                    acc = acc + dot(gates, jnp.concatenate([came[d, 0], came[d, 1]] * TERMS, axis=0))
                else:
                    acc = acc + inb[d, j - FAR]
                part[pos - 1, core, :, cols] = acc
            rs_copy(m, d, j).start()

    def finish(m, r):
        pos = HERE
        need_sib(m, pos)
        cols = pl.ds(r * half, half)
        acc = part[pos - 1, core, :, cols] + sib[m, pos - 1, :, cols]
        for d in range(2):
            j = SENDS - 2 if (r == 1) == (d == 0) else SENDS - 1
            if (m, d, j) not in seen:
                seen.add((m, d, j))
                rs_copy(m, d, j).wait_recv()
            acc = acc + inb[d, j - 2]
        rows = pl.ds(m * micro, micro)
        outv[rows, cols] = acc.astype(BF16)

    def combine_send(m, pos):
        combine(m, pos)
        sb_copy(m, pos).start()

    def combine_loop(m, first, last):
        @pl.loop(first, last)
        def _(pos):
            combine_send(m, pos)

    def part_free(m, pos):
        if pos == 0:
            landed(rows_sib, sb_s.at[pos])
            landed(rows_out.at[m], rs_s.at[pos])
        elif pos == HERE:
            landed(part.at[0, other], sb_s.at[pos])
        elif pos // 2 == 1:
            landed(part.at[1, other], sb_s.at[key(pos)])
            landed(part.at[1, core], rs_s.at[key(pos)])
            landed(near_out.at[m], nr_s)
            for d in range(2):
                landed(near_sib.at[d], nb_s.at[d])
        else:
            landed(part.at[pl.ds(pos - 1, 2), other], sb_s.at[key(pos)])
            landed(part.at[pl.ds(pos - 1, 2), core], rs_s.at[key(pos)])

    def pair_wait(m, p):
        landed(xg.at[m, p, pl.ds(0, chip)], dx_r.at[m, p])

    def info_wait(p):
        landed(meta.at[pl.ds(2 * p, 2), 0], dm_r.at[p])

    loads = [pltpu.make_async_copy(x_hbm.at[pl.ds(m * micro, micro)], x_rows(m, HERE, core, 0, micro), ld_sem.at[m])
             for m in range(2)]
    loads.append(pltpu.make_async_copy(ids_hbm, ids_v, ld_sem.at[2]))
    loads.append(pltpu.make_async_copy(rw_hbm, rw_v, ld_sem.at[3]))
    for cp in loads:
        cp.start()

    def enter():
        barrier = pltpu.get_barrier_semaphore()
        for dev in (nbr[0], nbr[1], sibling):
            pl.semaphore_signal(barrier, inc=1, device_id={'ep': dev}, device_id_type=MESH)
        pl.semaphore_wait(barrier, 3)

    enter()
    loads[0].wait()

    send_own(0, 0, 1)
    for cp in loads[2:]:
        cp.wait()
    loads[1].wait()
    make_meta()
    for d in range(2):
        mt_copy(d, 0).start()
    dm_copy(HERE, core).start()
    send_own(0, 1, PIECES)
    load_weights()

    def prepare(p):
        info_wait(p)
        index(0, p)

    def fetch(m, p):
        pair_wait(m, p)
        gather(m, p)

    near, mid, wide, far = 3, 2, 1, 0
    gates_ahead = functools.partial(index_far, 0)
    mt_event(0)
    take(0, 0, PIECES)
    n = PIECES
    mt_event(1)
    take(0, n)
    prepare(near)
    take(0, n + 1)
    take(0, n + 2)
    prepare(mid)
    take(0, n + 3)
    gates_ahead(0, 1)
    pair_wait(0, near)
    n += PIECES
    mt_event(2)
    take(0, n)
    gather(0, near)
    gates_ahead(1, 1)
    take(0, n + 1)
    send_own(1, 0, PIECES)
    index(1, near)
    take(0, n + 2)
    prepare(wide)
    gates_ahead(0, 0)
    take(0, n + 3)
    fetch(0, mid)
    n += PIECES
    mt_event(last)
    gates_ahead(1, 0)
    take(0, n)
    prepare(far)
    take(0, n + 1)
    pl.when(core == 1)(functools.partial(take, 1, 0))
    fetch(0, wide)
    fetch(0, far)
    pl.when(core == 1)(functools.partial(take, 1, 1))

    due = {}
    for c, first, steps in ((0, 0, (0, 1, 2, 4, 5, 6, 8, 9, 10, 11)), (1, 2, (0, 1, 2, 4, 5, 6, 8, 9))):
        for n, step in enumerate(steps, first):
            due[divmod(step, STEPS) + (c,)] = functools.partial(take, 1, n)
    experts(0, due)
    far_rows(0)
    near_rows(0)
    combine_send(0, 2)
    back(0, 0)
    combine_send(0, 3)
    n = (last - 1) * PIECES + 2
    take(1, n, 2)
    back(0, 1)
    combine_loop(0, FAR, FAR + 2)
    take(1, last * PIECES, 2)
    combine_loop(0, FAR + 2, CHIPS)
    combine_send(0, HERE)
    for p in (mid, wide, far):
        index(1, p)
    for p in range(PAIRS):
        fetch(1, p)

    for j in range(2, SENDS):
        for d in range(2):
            need_sib(0, back_item(d, j)[0])

    back(0, 2)
    experts(1, {
        (1, 0): functools.partial(back, 0, 3),
        (2, 2): functools.partial(back, 0, 4),
    })
    part_free(0, 0)
    far_rows(1)
    part_free(0, 2)
    near_rows(1)
    for i in range(FAR):
        index_far(1, i // 2, i % 2)
    combine_send(1, 2)
    combine_send(1, 3)
    back(0, 5)
    back(0, 6)
    back(1, 0)
    back(1, 1)
    finish(0, 0)
    finish(0, 1)
    for pos in (HERE, *range(FAR, CHIPS, 2)):
        part_free(0, pos)
    combine_loop(1, FAR, CHIPS)
    combine_send(1, HERE)
    for j in range(2, SENDS):
        back(1, j)
    finish(1, 0)
    finish(1, 1)

    def drain():
        for m in range(2):
            for d in range(2):
                landed(xg.at[m, 0, pl.ds(0, (3 * PIECES + PIECES // 2) * piece_rows)], ag_s.at[m, d])
            landed(xg.at[m, pl.ds(0, 2)], dx_s.at[m])
        landed(meta.at[pl.ds(0, 7), 0], mt_s)
        landed(meta.at[pl.ds(0, 8), 0], dm_s)
        for pos in (0, HERE, *range(2, CHIPS, 2)):
            part_free(1, pos)

    drain()


def solution(mesh):
    group = mesh.shape['ep']

    def device_fn(act_in, router_w, expert_ids, w_gate, w_up, w_down):
        tokens, dim = act_in.shape
        local_experts, _, ffn = w_gate.shape
        micro = tokens // 2
        mean_load = micro * expert_ids.shape[1] // (local_experts * group)
        cap = mean_load + mean_load // 2
        slots = 4 * cap
        rows = local_experts * cap
        dma = pltpu.SemaphoreType.DMA
        both = (2, 2)
        scratch = [
            pltpu.VMEM((2, 4, 4 * micro, dim), BF16),
            pltpu.VMEM((CHIPS, *both, 16, 2 * micro), F32),
            pltpu.VMEM(expert_ids.shape[::-1], jnp.int32),
            pltpu.VMEM((local_experts, 4 * slots, dim), BF16),
            pltpu.VMEM((4 * slots, ffn), BF16),
            pltpu.VMEM((4, local_experts * slots, dim), BF16),
            pltpu.VMEM((4, local_experts * slots, 4 * micro), BF16),
            pltpu.VMEM((2, 4, 4 * micro, 3 * local_experts * slots), BF16),
            pltpu.VMEM((*both, 2 * micro, 2 * TERMS * rows), BF16),
            pltpu.VMEM((*both, rows, dim), BF16),
            pltpu.VMEM((rows, dim), BF16),
            pltpu.VMEM((*both, rows, dim // 2), BF16),
            pltpu.VMEM((*both, 2, rows, dim // 2), BF16),
            pltpu.VMEM((2, rows, dim // 2), BF16),
            pltpu.VMEM((*both, rows, dim // 2), BF16),
            pltpu.VMEM((CHIPS - 1, 2, micro, dim), F32),
            pltpu.VMEM((2, CHIPS - 1, micro, dim), F32),
            pltpu.VMEM((2, SENDS - 2, micro, dim // 2), F32),
            pltpu.VMEM((*both, 2, dim, GU_TILE), BF16),
            pltpu.VMEM((2, ffn, dim), BF16),
            dma(both), dma((2, 4, PIECES)),
            dma((2,)), dma((2, 4)),
            dma, dma((2, 4)),
            dma, dma((4,)),
            dma((5,)),
            dma((5,)), dma((2, 5)),
            dma, dma((2,)), dma(both),
            dma(both), dma((2,)), dma((4,)),
        ]
        return pl.pallas_call(
            functools.partial(layer_kernel, group),
            out_shape=pltpu.VMEM((tokens, dim), BF16),
            in_specs=[pl.BlockSpec(memory_space=pl.ANY)] * 6,
            out_specs=pl.BlockSpec(memory_space=pltpu.VMEM),
            scratch_shapes=scratch,
            compiler_params=pltpu.CompilerParams(collective_id=0, has_side_effects=True,
                                                 vmem_limit_bytes=66453504),
            name='moe_layer',
        )(expert_ids.T, router_w.T, act_in, w_gate, w_up, w_down)

    row_spec = P(('dp', 'ep'), None)
    expert_spec = P('ep', None, None)
    return jax.shard_map(device_fn, mesh=mesh,
                         in_specs=(row_spec, P(None, None), row_spec, expert_spec, expert_spec, expert_spec),
                         out_specs=row_spec, check_vma=False)
```

```python
import functools

import jax
import jax.numpy as jnp
from jax import lax
from jax.experimental import pallas as pl
from jax.experimental.pallas import tpu as pltpu
from jax.sharding import PartitionSpec as P

MESH = pl.DeviceIdType.MESH
F32 = jnp.float32
BF16 = jnp.bfloat16

FAR = 4
ORDER = (FAR, 0, -3, 3, -2, 2, -1, 1)
POS = {away: i for i, away in enumerate(ORDER)}
POS[-FAR] = POS[FAR]
HERE = POS[0]
CHIPS = len(ORDER)
PAIRS = CHIPS // 2
SIGN = (1, -1)
TERMS = 3
NT = (((1,), (1,)), ((), ()))
BACK = ((FAR, 0),) + tuple((away, r) for away in range(FAR - 1, 0, -1) for r in (1, 0))
SENDS = len(BACK)
STEPS = 3
GU_TILE = 512
WIDE = 512
MXU = 256
PIECES = 4


def dot(a, b):
    return jnp.dot(a, b, preferred_element_type=F32)


def layer_kernel(group, ids_hbm, rw_hbm, x_hbm, wg_hbm, wu_hbm, wd_hbm, outv,
                 xg, meta, ids_v, xe, hid, eo, picks, cm, fm, rows_out, rows_sib, rows_in, near_out, near_sib, near_in, part, sib, inb, wgu, wdn,
                 ag_s, ag_r, dx_s, dx_r, mt_s, mt_r, dm_s, dm_r, rs_s, sb_s, sb_r, nr_s, nb_s, nb_r,
                 gu_sem, dn_sem, ld_sem):
    micro = outv.shape[0] // 2
    chip = 2 * micro
    dim = outv.shape[1]
    half = dim // 2
    last = FAR - 1
    piece_rows = micro // PIECES
    me = lax.axis_index('ep')
    core = lax.rem(me, 2)
    other = 1 - core
    nbr = (lax.rem(me + 2, group), lax.rem(me + group - 2, group))
    sibling = me + 1 - 2 * core
    local_experts = wg_hbm.shape[0]
    slots = xe.shape[1] // PAIRS
    cap = slots // (2 * 2)

    def remote(src, dst, ssem, rsem, dev):
        return pltpu.make_async_remote_copy(src_ref=src, dst_ref=dst, send_sem=ssem, recv_sem=rsem,
                                            device_id={'ep': dev}, device_id_type=MESH)

    def gu_copies(e, f):
        cols = pl.ds(f * GU_TILE, GU_TILE)
        s = lax.rem(e, 2)
        return (pltpu.make_async_copy(wg_hbm.at[e, :, cols], wgu.at[s, f, 0], gu_sem.at[s, f]),
                pltpu.make_async_copy(wu_hbm.at[e, :, cols], wgu.at[s, f, 1], gu_sem.at[s, f]))

    def dn_copy(e):
        return pltpu.make_async_copy(wd_hbm.at[e], wdn.at[lax.rem(e, 2)], dn_sem.at[lax.rem(e, 2)])

    def load_weights():
        for e in range(2):
            for f in range(2):
                for cp in gu_copies(e, f):
                    cp.start()
            dn_copy(e).start()

    def x_rows(m, pos, c, start, size):
        row = pl.multiple_of((pos % 2) * chip + c * micro + start, 16)
        return xg.at[m, pos // 2, pl.ds(row, size)]

    def ag_copy(m, d, k, i):
        start = ((i + d * PIECES // 2) % PIECES) * piece_rows
        src = x_rows(m, POS[-SIGN[d] * k], core, start, piece_rows)
        dst = x_rows(m, POS[-SIGN[d] * (k + 1)], core, start, piece_rows)
        return remote(src, dst, ag_s.at[m, d], ag_r.at[d, k, i], nbr[d])

    def ag_has(k, i):
        return k < last or i < PIECES // 2

    def landed(ref, sem):
        pltpu.make_async_copy(ref, ref, sem).wait()

    def dx_copy(m, pos, c):
        ref = x_rows(m, pos, c, 0, micro)
        return remote(ref, ref, dx_s.at[m], dx_r.at[m, pos // 2], sibling)

    def mt_copy(d, k):
        return remote(meta.at[POS[-SIGN[d] * k], core], meta.at[POS[-SIGN[d] * (k + 1)], core],
                      mt_s, mt_r.at[d, k], nbr[d])

    def mt_has(d, k):
        return k < last or d == 0

    def dm_copy(pos, c):
        return remote(meta.at[pos, c], meta.at[pos, c], dm_s, dm_r.at[pos // 2], sibling)

    def send_own(m, first, last):
        for i in range(first, last):
            for d in range(2):
                ag_copy(m, d, 0, i).start()
        if last == PIECES:
            dx_copy(m, HERE, core).start()

    def ag_event(m, k, i):
        for d in range(2):
            ag_copy(m, d, k, i).wait_recv()
            if k < last and ag_has(k + 1, i):
                ag_copy(m, d, k + 1, i).start()
        if k == last:
            for d in range(2):
                ref = x_rows(m, POS[FAR], core, (i + d * PIECES // 2) * piece_rows, piece_rows)
                remote(ref, ref, dx_s.at[m], dx_r.at[m, POS[FAR] // 2], sibling).start()
        elif i + 1 == PIECES:
            for d in range(2):
                dx_copy(m, POS[-SIGN[d] * (k + 1)], core).start()

    def take(m, first, count=1):
        for n in range(first, first + count):
            ag_event(m, n // PIECES, n % PIECES)

    def mt_event(k):
        for d in range(2):
            if mt_has(d, k):
                mt_copy(d, k).wait_recv()
                if k < last and mt_has(d, k + 1):
                    mt_copy(d, k + 1).start()
                dm_copy(POS[-SIGN[d] * (k + 1)], core).start()

    rw_v = xe.at[local_experts - 1, pl.ds(0, rw_hbm.shape[0])]

    def make_meta():
        for m in range(2):
            rows = x_rows(m, HERE, core, 0, micro)
            part[0, m, :, 0:rw_v.shape[0]] = lax.dot_general(rows[...], rw_v[...], NT, preferred_element_type=F32)
        ids = ids_v[...].astype(F32)
        expert = lax.broadcasted_iota(jnp.int32, (rw_v.shape[0], chip), 0).astype(F32)
        logits = jnp.concatenate([part[0, m, :, 0:chip] for m in range(2)], axis=0).T[0:rw_v.shape[0]]
        picked = []
        for j in range(8):
            picked.append(jnp.sum(jnp.where(expert == ids[j:j + 1], logits, 0.0), axis=0, keepdims=True))
        picked = jnp.concatenate(picked, axis=0)
        top = jnp.exp(picked - jnp.max(picked, axis=0, keepdims=True))
        gates = top / jnp.sum(top, axis=0, keepdims=True)
        both = jnp.concatenate([ids, gates], axis=0)
        turned = pltpu.roll(both, micro, 1)
        mine = lax.broadcasted_iota(jnp.int32, both.shape, 1) // micro == core
        for m in range(2):
            meta[HERE, core, m] = jnp.where(mine, jnp.where(core == m, both, turned), 0.0)

    def grid(shape, axis):
        return lax.broadcasted_iota(jnp.int32, shape, axis)

    def one(mask):
        return jnp.where(mask, 1.0, 0.0).astype(BF16)

    def chip_info(pos, m):
        return meta[pos, 0, m] + meta[pos, 1, m]

    def places(info, first, count):
        token = info.shape[1]
        ids, gates = jnp.split(info, 2)
        chosen, weight = [], []
        for e in range(count):
            hit = ids == (first + e).astype(F32)
            chosen.append(jnp.sum(jnp.where(hit, 1.0, 0.0), axis=0, keepdims=True))
            weight.append(jnp.sum(jnp.where(hit, gates, 0.0), axis=0, keepdims=True))
        stacked = jnp.concatenate(chosen + [jnp.zeros((info.shape[0] - count, token), F32)], axis=0)
        row, col = grid((token, token), 0), grid((token, token), 1)
        rank = dot(stacked.astype(BF16), one((row < col) & (row // micro == col // micro)))
        return [jnp.where(chosen[e] > 0.5, rank[e:e + 1], -slots) for e in range(count)], weight, one(row == col)

    def three_terms(rest):
        terms = []
        for i in range(TERMS):
            terms.append(rest.astype(BF16))
            rest = rest - terms[i].astype(F32)
        return jnp.concatenate(terms, axis=0)

    def index(m, p):
        info = jnp.concatenate([chip_info(2 * p, m), chip_info(2 * p + 1, m)], axis=1)
        place, weight, eye = places(info, me * local_experts, local_experts)
        slot = grid((slots, 2 * chip), 0) - grid((slots, 2 * chip), 1) // micro * cap
        slot = slot.astype(F32)
        at = [slot == place[e] for e in range(local_experts)]
        picks[p] = jnp.concatenate([jnp.where(a, 1.0, 0.0) for a in at], axis=0).astype(BF16)
        mix = jnp.concatenate([jnp.where(at[e], weight[e], 0.0) for e in range(local_experts)], axis=0)
        cm[m, p] = lax.dot_general(eye, three_terms(mix), NT, preferred_element_type=F32).astype(BF16)

    def index_far(m, d, step):
        count = 2 * local_experts
        home = POS[SIGN[d] * (FAR - 1 - step)]
        first = lax.rem(me - core + group - 2 * SIGN[d], group) * local_experts
        place, weight, eye = places(chip_info(home, m), first, count)
        slot = grid((16, chip), 0).astype(F32)
        mix = jnp.concatenate([jnp.where(slot == place[e], weight[e], 0.0) for e in range(count)], axis=0)
        turned = lax.dot_general(eye, three_terms(mix), NT, preferred_element_type=F32).astype(BF16)
        wide, tight = 16 * count, cap * count
        row, col = grid((TERMS * wide, TERMS * tight), 0), grid((TERMS * wide, TERMS * tight), 1)
        i = col % tight
        fm[step, d] = dot(turned, one((row // wide == col // tight) & (row % wide == i // cap * 16 + i % cap))).astype(BF16)

    def gather(m, p):
        for n in range(0, dim, WIDE):
            rows = dot(picks[p], xg[m, p, :, n:n + WIDE]).astype(BF16)
            for e in range(local_experts):
                xe[e, pl.ds(pl.multiple_of(p * slots, 16), slots), n:n + WIDE] = rows[e * slots:(e + 1) * slots]

    def experts(m, service):
        @pl.loop(0, local_experts)
        def _(e):
            s = lax.rem(e, 2)
            nxt = lax.rem(e + 2, local_experts)

            def after(step, copies):
                def start():
                    for cp in copies:
                        cp.start()

                if m == 0:
                    start()
                else:
                    pl.when(e + 2 < local_experts)(start)
                for at, fn in service.items():
                    if at[1] == step:
                        who = functools.reduce(lambda x, c: x & (core == c), at[2:], e == at[0])
                        pl.when(who)(fn)

            for f in range(2):
                landed(wgu.at[s, f], gu_sem.at[s, f])
                for c in range(0, GU_TILE, MXU):
                    a = dot(xe[e], wgu[s, f, 0, :, c:c + MXU])
                    b = dot(xe[e], wgu[s, f, 1, :, c:c + MXU])
                    hid[:, f * GU_TILE + c:f * GU_TILE + c + MXU] = (a * jax.nn.sigmoid(a) * b).astype(BF16)
                after(f, gu_copies(nxt, f))
            dn_copy(e).wait()
            for c in range(0, dim, MXU):
                o = dot(hid[...], wdn[s, :, c:c + MXU]).astype(BF16)
                for p in range(4):
                    eo[p, pl.ds(pl.multiple_of(e * slots, 16), slots), c:c + MXU] = o[p * slots:(p + 1) * slots]
            after(2, (dn_copy(nxt),))

    def sum_cols(pos):
        if isinstance(pos, int) and pos // 2 == 1:
            first = back_item(1 - pos % 2, 2)[1] * half
            return first, first + half
        return 0, dim

    def combine(m, pos):
        p, top = pos // 2, (pos % 2) * chip
        if not isinstance(pos, int):
            top = pl.multiple_of(top, chip)
        gates = cm[m, p, pl.ds(top, chip)]
        first, after = sum_cols(pos)
        for n in range(first, after, WIDE):
            o = eo[p, :, n:n + WIDE]
            acc = dot(gates, jnp.concatenate([o, o, o], axis=0))
            part[pos - 1, 0, :, n:n + WIDE] = acc[:micro]
            part[pos - 1, 1, :, n:n + WIDE] = acc[micro:]

    def raw_rows(pos, first, after, own, sent):
        count = local_experts * cap
        shape = (2 * count, local_experts * slots)
        row, col = grid(shape, 0), grid(shape, 1)
        i = row % count
        owner = jnp.where(row < count, core, other) + pos % 2 * 2
        take_row = one(col == i // cap * slots + owner * cap + i % cap)
        for n in range(first, after, WIDE):
            o = dot(take_row, eo[pos // 2, :, n:n + WIDE]).astype(BF16)
            own[:, n - first:n - first + WIDE] = o[:count]
            sent[:, n - first:n - first + WIDE] = o[count:]

    def far_rows(m):
        raw_rows(0, 0, dim, rows_out.at[m, core], rows_sib)
        sb_copy(m, 0).start()

    def near_rows(m):
        for d in range(2):
            pos, r = back_item(d, 1)
            raw_rows(pos, r * half, r * half + half, near_out.at[m, d, core], near_sib.at[d])
            remote(near_sib.at[d], near_out.at[m, d, core], nb_s.at[d], nb_r.at[m, d], sibling).start()

    def key(pos):
        return pos if isinstance(pos, int) and pos < 2 else pos // 2 + 1

    def sb_copy(m, pos):
        if isinstance(pos, int) and pos == 0:
            return remote(rows_sib, rows_out.at[m, core], sb_s.at[key(pos)], sb_r.at[m, key(pos)], sibling)
        if isinstance(pos, int):
            first, after = sum_cols(pos)
            cols = pl.ds(first, after - first)
            return remote(part.at[pos - 1, other, :, cols], sib.at[m, pos - 1, :, cols],
                          sb_s.at[key(pos)], sb_r.at[m, key(pos)], sibling)
        return remote(part.at[pos - 1, other], sib.at[m, pos - 1], sb_s.at[key(pos)], sb_r.at[m, key(pos)], sibling)

    def back_item(d, j):
        dist, cols = BACK[j]
        return POS[SIGN[d] * dist], (cols if d == 0 else 1 - cols)

    def rs_copy(m, d, j):
        pos, r = back_item(d, j)
        cols = pl.ds(r * half, half)
        if j == 0:
            return remote(rows_out.at[m, :, :, cols], rows_in.at[d], rs_s.at[key(pos)], ag_r.at[d, j // PIECES, j % PIECES], nbr[d])
        if j == 1:
            return remote(near_out.at[m, d], near_in.at[d], nr_s, ag_r.at[d, j // PIECES, j % PIECES], nbr[d])
        return remote(part.at[pos - 1, core, :, cols], inb.at[d, j - 2], rs_s.at[key(pos)], ag_r.at[d, j // PIECES, j % PIECES], nbr[d])

    seen = set()

    def need_sib(m, pos):
        if (m, key(pos)) not in seen:
            seen.add((m, key(pos)))
            if pos == 0:
                came = rows_out.at[m, other]
            elif pos == HERE:
                came = sib.at[m, 0]
            elif pos // 2 == 1:
                came = sib.at[m, 1]
            else:
                came = sib.at[m, pl.ds(pos - pos % 2 - 1, 2)]
            landed(came, sb_r.at[m, key(pos)])

    def back(m, j):
        for d in range(2):
            pos, r = back_item(d, j)
            if j == 1:
                landed(near_out.at[m, d, other], nb_r.at[m, d])
            else:
                need_sib(m, pos)
            if j > 1:
                cols = pl.ds(r * half, half)
                acc = part[pos - 1, core, :, cols] + sib[m, pos - 1, :, cols]
                rs_copy(m, d, j - 2).wait_recv()
                if j < FAR:
                    gates = fm[j - 2, d, pl.ds(pl.multiple_of(core * micro, micro), micro)]
                    came = near_in if j == last else rows_in
                    acc = acc + dot(gates, jnp.concatenate([came[d, 0], came[d, 1]] * TERMS, axis=0))
                else:
                    acc = acc + inb[d, j - FAR]
                part[pos - 1, core, :, cols] = acc
            rs_copy(m, d, j).start()

    def finish(m, r):
        pos = HERE
        need_sib(m, pos)
        cols = pl.ds(r * half, half)
        acc = part[pos - 1, core, :, cols] + sib[m, pos - 1, :, cols]
        for d in range(2):
            j = SENDS - 2 if (r == 1) == (d == 0) else SENDS - 1
            if (m, d, j) not in seen:
                seen.add((m, d, j))
                rs_copy(m, d, j).wait_recv()
            acc = acc + inb[d, j - 2]
        rows = pl.ds(m * micro, micro)
        outv[rows, cols] = acc.astype(BF16)

    def combine_send(m, pos):
        combine(m, pos)
        sb_copy(m, pos).start()

    def combine_loop(m, first, last):
        @pl.loop(first, last)
        def _(pos):
            combine_send(m, pos)

    def part_free(m, pos):
        if pos == 0:
            landed(rows_sib, sb_s.at[pos])
            landed(rows_out.at[m], rs_s.at[pos])
        elif pos == HERE:
            landed(part.at[0, other], sb_s.at[pos])
        elif pos // 2 == 1:
            landed(part.at[1, other], sb_s.at[key(pos)])
            landed(part.at[1, core], rs_s.at[key(pos)])
            landed(near_out.at[m], nr_s)
            for d in range(2):
                landed(near_sib.at[d], nb_s.at[d])
        else:
            landed(part.at[pl.ds(pos - 1, 2), other], sb_s.at[key(pos)])
            landed(part.at[pl.ds(pos - 1, 2), core], rs_s.at[key(pos)])

    def pair_wait(m, p):
        landed(xg.at[m, p, pl.ds(0, chip)], dx_r.at[m, p])

    def info_wait(p):
        landed(meta.at[pl.ds(2 * p, 2), 0], dm_r.at[p])

    loads = [pltpu.make_async_copy(x_hbm.at[pl.ds(m * micro, micro)], x_rows(m, HERE, core, 0, micro), ld_sem.at[m])
             for m in range(2)]
    loads.append(pltpu.make_async_copy(ids_hbm, ids_v, ld_sem.at[2]))
    loads.append(pltpu.make_async_copy(rw_hbm, rw_v, ld_sem.at[3]))
    for cp in loads:
        cp.start()

    def enter():
        barrier = pltpu.get_barrier_semaphore()
        for dev in (nbr[0], nbr[1], sibling):
            pl.semaphore_signal(barrier, inc=1, device_id={'ep': dev}, device_id_type=MESH)
        pl.semaphore_wait(barrier, 3)

    enter()
    loads[0].wait()

    send_own(0, 0, 1)
    for cp in loads[2:]:
        cp.wait()
    loads[1].wait()
    make_meta()
    for d in range(2):
        mt_copy(d, 0).start()
    dm_copy(HERE, core).start()
    send_own(0, 1, PIECES)
    load_weights()

    def prepare(p):
        info_wait(p)
        index(0, p)

    def fetch(m, p):
        pair_wait(m, p)
        gather(m, p)

    near, mid, wide, far = 3, 2, 1, 0
    gates_ahead = functools.partial(index_far, 0)
    mt_event(0)
    take(0, 0, PIECES)
    n = PIECES
    mt_event(1)
    take(0, n)
    prepare(near)
    take(0, n + 1)
    take(0, n + 2)
    prepare(mid)
    take(0, n + 3)
    gates_ahead(0, 1)
    pair_wait(0, near)
    n += PIECES
    mt_event(2)
    take(0, n)
    gather(0, near)
    gates_ahead(1, 1)
    take(0, n + 1)
    send_own(1, 0, PIECES)
    index(1, near)
    take(0, n + 2)
    prepare(wide)
    gates_ahead(0, 0)
    take(0, n + 3)
    fetch(0, mid)
    n += PIECES
    mt_event(last)
    gates_ahead(1, 0)
    take(0, n)
    prepare(far)
    take(0, n + 1)
    pl.when(core == 1)(functools.partial(take, 1, 0))
    fetch(0, wide)
    fetch(0, far)
    pl.when(core == 1)(functools.partial(take, 1, 1))

    due = {}
    for c, first, steps in ((0, 0, (0, 1, 2, 4, 5, 6, 8, 9, 10, 11)), (1, 2, (0, 1, 2, 4, 5, 6, 8, 9))):
        for n, step in enumerate(steps, first):
            due[divmod(step, STEPS) + (c,)] = functools.partial(take, 1, n)
    experts(0, due)
    far_rows(0)
    near_rows(0)
    back(0, 0)
    combine_send(0, 2)
    combine_send(0, 3)
    n = (last - 1) * PIECES + 2
    take(1, n, 2)
    back(0, 1)
    combine_loop(0, FAR, FAR + 2)
    take(1, last * PIECES, 2)
    combine_loop(0, FAR + 2, CHIPS)
    combine_send(0, HERE)
    for p in (mid, wide, far):
        index(1, p)
    for p in range(PAIRS):
        fetch(1, p)

    for j in range(2, SENDS):
        for d in range(2):
            need_sib(0, back_item(d, j)[0])

    back(0, 2)
    experts(1, {
        (1, 0): functools.partial(back, 0, 3),
        (2, 2): functools.partial(back, 0, 4),
    })
    part_free(0, 0)
    far_rows(1)
    part_free(0, 2)
    near_rows(1)
    for i in range(FAR):
        index_far(1, i // 2, i % 2)
    combine_send(1, 2)
    combine_send(1, 3)
    back(0, 5)
    back(0, 6)
    back(1, 0)
    back(1, 1)
    finish(0, 0)
    finish(0, 1)
    for pos in (HERE, *range(FAR, CHIPS, 2)):
        part_free(0, pos)
    combine_loop(1, FAR, CHIPS)
    combine_send(1, HERE)
    for j in range(2, SENDS):
        back(1, j)
    finish(1, 0)
    finish(1, 1)

    def drain():
        for m in range(2):
            for d in range(2):
                landed(xg.at[m, 0, pl.ds(0, (3 * PIECES + PIECES // 2) * piece_rows)], ag_s.at[m, d])
            landed(xg.at[m, pl.ds(0, 2)], dx_s.at[m])
        landed(meta.at[pl.ds(0, 7), 0], mt_s)
        landed(meta.at[pl.ds(0, 8), 0], dm_s)
        for pos in (0, HERE, *range(2, CHIPS, 2)):
            part_free(1, pos)

    drain()


def solution(mesh):
    group = mesh.shape['ep']

    def device_fn(act_in, router_w, expert_ids, w_gate, w_up, w_down):
        tokens, dim = act_in.shape
        local_experts, _, ffn = w_gate.shape
        micro = tokens // 2
        mean_load = micro * expert_ids.shape[1] // (local_experts * group)
        cap = mean_load + mean_load // 2
        slots = 4 * cap
        rows = local_experts * cap
        dma = pltpu.SemaphoreType.DMA
        both = (2, 2)
        scratch = [
            pltpu.VMEM((2, 4, 4 * micro, dim), BF16),
            pltpu.VMEM((CHIPS, *both, 16, 2 * micro), F32),
            pltpu.VMEM(expert_ids.shape[::-1], jnp.int32),
            pltpu.VMEM((local_experts, 4 * slots, dim), BF16),
            pltpu.VMEM((4 * slots, ffn), BF16),
            pltpu.VMEM((4, local_experts * slots, dim), BF16),
            pltpu.VMEM((4, local_experts * slots, 4 * micro), BF16),
            pltpu.VMEM((2, 4, 4 * micro, 3 * local_experts * slots), BF16),
            pltpu.VMEM((*both, 2 * micro, 2 * TERMS * rows), BF16),
            pltpu.VMEM((*both, rows, dim), BF16),
            pltpu.VMEM((rows, dim), BF16),
            pltpu.VMEM((*both, rows, dim // 2), BF16),
            pltpu.VMEM((*both, 2, rows, dim // 2), BF16),
            pltpu.VMEM((2, rows, dim // 2), BF16),
            pltpu.VMEM((*both, rows, dim // 2), BF16),
            pltpu.VMEM((CHIPS - 1, 2, micro, dim), F32),
            pltpu.VMEM((2, CHIPS - 1, micro, dim), F32),
            pltpu.VMEM((2, SENDS - 2, micro, dim // 2), F32),
            pltpu.VMEM((*both, 2, dim, GU_TILE), BF16),
            pltpu.VMEM((2, ffn, dim), BF16),
            dma(both), dma((2, 4, PIECES)),
            dma((2,)), dma((2, 4)),
            dma, dma((2, 4)),
            dma, dma((4,)),
            dma((5,)),
            dma((5,)), dma((2, 5)),
            dma, dma((2,)), dma(both),
            dma(both), dma((2,)), dma((4,)),
        ]
        return pl.pallas_call(
            functools.partial(layer_kernel, group),
            out_shape=pltpu.VMEM((tokens, dim), BF16),
            in_specs=[pl.BlockSpec(memory_space=pl.ANY)] * 6,
            out_specs=pl.BlockSpec(memory_space=pltpu.VMEM),
            scratch_shapes=scratch,
            compiler_params=pltpu.CompilerParams(collective_id=0, has_side_effects=True,
                                                 vmem_limit_bytes=66453504),
            name='moe_layer',
        )(expert_ids.T, router_w.T, act_in, w_gate, w_up, w_down)

    row_spec = P(('dp', 'ep'), None)
    expert_spec = P('ep', None, None)
    return jax.shard_map(device_fn, mesh=mesh,
                         in_specs=(row_spec, P(None, None), row_spec, expert_spec, expert_spec, expert_spec),
                         out_specs=row_spec, check_vma=False)
```
